128 devices in a mesh: fit: 1, comp: 2 (over core), pts: 64 (over z, y, x).
Axes of the slice: x: 4, y: 4, z: 4, core: 2. Of those that a mesh axis runs over, the one named last changes fastest.
Arguments:
- points: bfloat16 [262144, 512], P(('fit', 'pts'))
- means_init: float32 [4096, 512], P(('fit', 'comp'))
- logw_init: float32 [4096], P(('fit', 'comp'))
- inv_temp: float32 [3], replicated
Outputs:
- output 1: float32 [4096, 512], P(('fit', 'comp'))
- output 2: float32 [4096], P(('fit', 'comp'))
- output 3: float32 [262144], P(('fit', 'pts'))
All inputs are finite; a program needn't handle non-finite values.
Results may differ from the reference program's by a relative error of at most 0.001.
Values are sent between devices in bfloat16 or wider.
A program may use at most 1 GiB of HBM per device.

```python
import jax
import jax.numpy as jnp
from jax import lax

N = 262144
K = 4096
D = 512
SWEEPS = 3
NUM_SRC = 256
ROW_BLOCK = 1024

PRIOR_ALPHA = 1e-3
COUNT_EPS = 1e-6


def setup_inputs(seed: int = 0, part: int = 0) -> dict:
    root_key = jax.random.key(seed)
    part_key = jax.random.fold_in(root_key, part)
    key_cent, key_noise, key_assign, key_mnoise, key_logw = jax.random.split(part_key, 5)
    key_temp = jax.random.fold_in(root_key, 1000003)
    center_std = (2.0 / D ** 0.5) ** 0.5
    centers = center_std * jax.random.normal(key_cent, (NUM_SRC, D), jnp.float32)
    src_id = (jnp.arange(N, dtype=jnp.int32) * NUM_SRC) // N
    points = centers[src_id] + jax.random.normal(key_noise, (N, D), jnp.float32)
    assign = jax.random.randint(key_assign, (K,), 0, NUM_SRC)
    means_init = centers[assign] + 0.8 * jax.random.normal(key_mnoise, (K, D), jnp.float32)
    logw_init = jax.nn.log_softmax(0.5 * jax.random.normal(key_logw, (K,), jnp.float32))
    temp_steps = jax.random.uniform(key_temp, (SWEEPS,), jnp.float32)
    inv_temp = (0.25 + 0.2 * jnp.cumsum(temp_steps)) / D ** 0.5
    return {"points": points.astype(jnp.bfloat16), "means_init": means_init, "logw_init": logw_init, "inv_temp": inv_temp}


def em_sweep(points, mean_vecs, log_w, temp):
    mean_bf = mean_vecs.astype(jnp.bfloat16)
    mean_sq = jnp.sum(mean_vecs * mean_vecs, axis=1)
    row_blocks = points.reshape(N // ROW_BLOCK, ROW_BLOCK, D)

    def scan_body(state_pair, row_blk):
        counts, stat_sums = state_pair
        x_sq = jnp.sum(jnp.square(row_blk.astype(jnp.float32)), axis=1)
        cross_dot = jnp.dot(row_blk, mean_bf.T, preferred_element_type=jnp.float32)
        logits = log_w[None, :] - temp * (x_sq[:, None] - 2.0 * cross_dot + mean_sq[None, :])
        row_top = jnp.max(logits, axis=1)
        exp_total = jnp.sum(jnp.exp(logits - row_top[:, None]), axis=1)
        log_norm = row_top + jnp.log(exp_total)
        resp_prob = jnp.exp(logits - log_norm[:, None])
        counts = counts + jnp.sum(resp_prob, axis=0)
        stat_sums = stat_sums + jnp.dot(resp_prob.astype(jnp.bfloat16).T, row_blk, preferred_element_type=jnp.float32)
        return (counts, stat_sums), log_norm

    init_state = (jnp.zeros((K,), jnp.float32), jnp.zeros((K, D), jnp.float32))
    (counts, stat_sums), log_norm = lax.scan(scan_body, init_state, row_blocks)
    new_means = stat_sums / (counts[:, None] + COUNT_EPS)
    new_logw = jnp.log((counts + PRIOR_ALPHA) / (N + K * PRIOR_ALPHA))
    return new_means, new_logw, log_norm.reshape(N)


def reference(points, means_init, logw_init, inv_temp):
    mean_vecs = means_init
    log_w = logw_init
    log_norm = jnp.zeros((N,), jnp.float32)
    for sweep_idx in range(SWEEPS):
        mean_vecs, log_w, log_norm = em_sweep(points, mean_vecs, log_w, inv_temp[sweep_idx])
    return mean_vecs, log_w, log_norm
```

```python
import functools
import math

import jax
import jax.numpy as jnp
from jax import lax
from jax.experimental import pallas as pl
from jax.experimental.pallas import tpu as pltpu
from jax.sharding import PartitionSpec as P

PRIOR_ALPHA = 1e-3
COUNT_EPS = 1e-6
LOG2E = math.log2(math.e)
LN2 = math.log(2.0)
F32, BF16 = jnp.float32, jnp.bfloat16
MESH = pl.DeviceIdType.MESH

AXES = {"z": 1, "y": 2, "x": 3}
ORDERS = (("x", "y", "z"), ("y", "z", "x"), ("z", "x", "y"))
SUM_TILES = ((0, 6), (6, 11), (11, 17))
BF_TILES = ((0, 3), (3, 6), (6, 8))
PB = 256
KC = 512


def cat(parts, axis):
    return jnp.concatenate(parts, axis=axis)


def kernel(n_total, k_total, sweeps, x_hbm, mu_hbm, ct_hbm, beta_ref, out_mu, out_ct, out_lse,
           xv, e_ref, l0, l1, s_ref, muf, mu, ct, hrep, lrep, st, stp, wrow, qh,
           ra0, ra1, ra2, rb0, rb1, rb2, rc0, rc1, rc2,
           load_sem, ex_send, ex_recv, rs_send, rs_recv, ag_send, ag_recv):
    n_pts = xv.shape[0]
    nb = n_pts // PB
    fit, comp, pts = lax.axis_index("fit"), lax.axis_index("comp"), lax.axis_index("pts")
    me = {"z": lax.div(pts, 16), "y": lax.rem(lax.div(pts, 4), 4), "x": lax.rem(pts, 4)}
    right = {d: lax.rem(me[d] + 1, 4) for d in me}
    left = {d: lax.rem(me[d] + 3, 4) for d in me}
    over = {d: lax.rem(me[d] + 2, 4) for d in me}
    bufs = ((ra0, ra1, ra2), (rb0, rb1, rb2), (rc0, rc1, rc2))

    def dev(d, v):
        c = dict(me)
        c[d] = v
        return (fit, comp, c["z"] * 16 + c["y"] * 4 + c["x"])

    def where_at(ts, sel):
        return (pl.ds(ts[0], ts[1] - ts[0]),) + tuple(sel.get(d, slice(None)) for d in ("z", "y", "x"))

    def remote(src, dst, ss, rs, device):
        return pltpu.make_async_remote_copy(src_ref=src, dst_ref=dst, send_sem=ss, recv_sem=rs,
                                            device_id=device, device_id_type=MESH)

    def half(i):
        return pl.ds(2 * i, 2)

    def reduce_phase(k):
        pend = []
        for p, order in enumerate(ORDERS):
            d, ts, buf = order[k], SUM_TILES[p], bufs[k][p]
            fixed = {order[j]: me[order[j]] for j in range(k)}

            def copy(i, src, device, p=p, buf=buf):
                c = remote(src, buf.at[i], rs_send.at[p, k, i], rs_recv.at[p, k, i], device)
                c.start()
                return c

            if k == 2:
                blk = lambda v, fixed=fixed, d=d, ts=ts: s_ref.at[where_at(ts, {**fixed, d: v})]
                cs = [copy(2, blk(over[d]), dev(d, over[d])), copy(0, blk(right[d]), dev(d, right[d])),
                      copy(1, blk(left[d]), dev(d, left[d]))]
                pend.append(cs)
                continue

            def at(v, h, fixed=fixed, d=d, ts=ts, order=order):
                return where_at(ts, {**fixed, d: v, order[2]: half(h)})

            to_r, to_l = dev(d, right[d]), dev(d, left[d])
            c0 = copy(0, s_ref.at[at(over[d], 0)], to_r)
            c1 = copy(1, s_ref.at[at(over[d], 1)], to_l)
            c3 = copy(3, s_ref.at[at(right[d], 1)], to_r)
            c4 = copy(4, s_ref.at[at(left[d], 0)], to_l)
            pend.append((c0, c1, c3, c4, at, copy))
        if k == 2:
            for p, order in enumerate(ORDERS):
                ts, buf = SUM_TILES[p], bufs[k][p]
                for c in pend[p]:
                    c.wait()
                own = where_at(ts, me)
                s_ref[own] = (s_ref[own] + buf[0]) + (buf[1] + buf[2])
            return
        fwd = []
        for p, order in enumerate(ORDERS):
            d, buf = order[k], bufs[k][p]
            c0, c1, c3, c4, at, copy = pend[p]
            c0.wait_recv()
            buf[0] = buf[0] + s_ref[at(right[d], 0)]
            c2 = copy(2, buf.at[0], dev(d, right[d]))
            c1.wait_recv()
            buf[1] = buf[1] + s_ref[at(left[d], 1)]
            c5 = copy(5, buf.at[1], dev(d, left[d]))
            fwd.append((c2, c5))
        for p, order in enumerate(ORDERS):
            d, buf = order[k], bufs[k][p]
            c0, c1, c3, c4, at, copy = pend[p]
            c2, c5 = fwd[p]
            c4.wait_recv()
            c2.wait_recv()
            s_ref[at(me[d], 0)] = s_ref[at(me[d], 0)] + (buf[2] + buf[4])
            c3.wait_recv()
            c5.wait_recv()
            s_ref[at(me[d], 1)] = s_ref[at(me[d], 1)] + (buf[3] + buf[5])
            for c in (c0, c1, c3, c4, c2, c5):
                c.wait_send()

    def gather_phase(k, blocks):
        def view(ref, ts, sel):
            w = where_at(ts or (0, 1), sel)
            return ref.at[w] if ts else ref.at[w[1:]]

        pend = []
        for p, order in enumerate(ORDERS):
            d = order[k]
            fixed = {order[j]: me[order[j]] for j in range(k)}
            for q, (ref, ts) in enumerate(blocks[p]):
                def copy(i, sel, device, p=p, q=q, ref=ref, ts=ts):
                    v = view(ref, ts, sel)
                    c = remote(v, v, ag_send.at[p, q, k, i], ag_recv.at[p, q, k, i], device)
                    c.start()
                    return c

                to_r, to_l, to_o = dev(d, right[d]), dev(d, left[d]), dev(d, over[d])
                if k == 2:
                    sel = {**fixed, d: me[d]}
                    pend.append((copy(0, sel, to_o), copy(1, sel, to_r), copy(2, sel, to_l)))
                    continue

                def sel(v, h, fixed=fixed, d=d, order=order):
                    return {**fixed, d: v, order[2]: half(h)}

                c0 = copy(0, sel(me[d], 0), to_r)
                c1 = copy(1, sel(me[d], 1), to_l)
                c2 = copy(2, sel(me[d], 1), to_r)
                c3 = copy(3, sel(me[d], 0), to_l)
                pend.append((d, c0, c1, c2, c3, sel, copy, to_r, to_l))
        if k == 2:
            for cs in pend:
                for c in cs:
                    c.wait()
            return
        fwd = []
        for d, c0, c1, c2, c3, sel, copy, to_r, to_l in pend:
            c0.wait_recv()
            c4 = copy(4, sel(left[d], 0), to_r)
            c1.wait_recv()
            c5 = copy(5, sel(right[d], 1), to_l)
            fwd.append((c4, c5))
        for (d, c0, c1, c2, c3, *_), (c4, c5) in zip(pend, fwd):
            for c in (c2, c3, c4, c5):
                c.wait_recv()
            for c in (c0, c1, c2, c3, c4, c5):
                c.wait_send()

    lane = lax.broadcasted_iota(jnp.int32, (8, 128), 1)

    def expand():
        t = ct[...].reshape(512, 128)
        for r4 in range(4):
            hrep[r4] = jnp.broadcast_to(t[:, 16 * r4:16 * r4 + 1], (512, 128))
            lrep[r4] = jnp.broadcast_to(t[:, 64 + 16 * r4:65 + 16 * r4], (512, 128)) * LOG2E

    def logits(j, lref, b2):
        cols = pl.ds(pl.multiple_of(j * PB, PB), PB)
        xj = xv[cols, :]
        q = qh[:, cols]
        top = None
        for r2 in range(2):
            rows = cat([mu[r2 * 4 + c].reshape(1024, 128) for c in range(4)], 1)
            a = lax.dot_general(rows, xj, (((1,), (1,)), ((), ())), preferred_element_type=F32)
            a = a.reshape(64, 2, 8, PB)
            for h in range(2):
                r4 = r2 * 2 + h
                hh = cat([hrep[r4]] * (PB // 128), 1)
                ll = cat([lrep[r4]] * (PB // 128), 1)
                v = ((a[:, h].reshape(512, PB) - hh) - q) * b2 + ll
                lref[r4] = v
                t = jnp.max(v.reshape(64, 8, PB), axis=0)
                top = t if top is None else jnp.maximum(top, t)
        st[0:1, cols] = jnp.max(top, axis=0, keepdims=True)

    def exps(j, lref):
        cols = pl.ds(pl.multiple_of(j * PB, PB), PB)
        m = st[0:1, cols]
        tot = None
        for r4 in range(4):
            e = jnp.exp2(lref[r4] - m)
            e_ref[r4, :, cols] = e
            t = jnp.sum(e.reshape(64, 8, PB), axis=0)
            tot = t if tot is None else tot + t
        st[1:2, cols] = jnp.sum(tot, axis=0, keepdims=True)

    cx = pltpu.make_async_copy(x_hbm, xv, load_sem.at[0])
    cm = pltpu.make_async_copy(mu_hbm, mu, load_sem.at[1])
    cc = pltpu.make_async_copy(ct_hbm, ct, load_sem.at[2])
    cx.start()
    cm.start()
    cc.start()
    cx.wait()
    cm.wait()
    cc.wait()

    @pl.loop(0, n_pts // 128)
    def _(i):
        rows = pl.ds(pl.multiple_of(i * 128, 128), 128)
        xb = xv[rows, :].astype(F32)
        sq = xb * xb
        sq = (sq[:, 0:128] + sq[:, 128:256]) + (sq[:, 256:384] + sq[:, 384:512])
        qh[:, rows] = jnp.sum(sq.T, axis=0, keepdims=True) * 0.5

    st[...] = jnp.zeros_like(st)

    @pl.loop(0, sweeps)
    def _(sweep):
        b2 = beta_ref[sweep] * (2.0 * LOG2E)
        expand()
        logits(0, l0, b2)

        @pl.loop(0, nb // 2 - 1)
        def _(i):
            logits(2 * i + 1, l1, b2)
            exps(2 * i, l0)
            logits(2 * i + 2, l0, b2)
            exps(2 * i + 1, l1)

        logits(nb - 1, l1, b2)
        exps(nb - 2, l0)
        exps(nb - 1, l1)

        slot = lax.rem(sweep, 2)
        ex = remote(st, stp.at[slot], ex_send, ex_recv.at[slot], (fit, 1 - comp, pts))
        ex.start()
        s_ref[16] = jnp.zeros((4, 4, 4, 8, 128), F32)
        ex.wait()
        ma, mb = st[0:1, :], stp[slot, 0:1, :]
        mm = jnp.maximum(ma, mb)
        tot = st[1:2, :] * jnp.exp2(ma - mm) + stp[slot, 1:2, :] * jnp.exp2(mb - mm)
        lse2 = mm + jnp.log2(tot)
        wrow[...] = jnp.exp2(ma - lse2)
        out_lse[...] = lse2 * LN2

        @pl.loop(0, 4)
        def _(r4):
            acc, cnt = None, None
            for kc in range(n_pts // KC):
                k0 = kc * KC
                r = e_ref[r4, :, k0:k0 + KC] * wrow[:, k0:k0 + KC]
                for t in range(KC // 128):
                    rt = r[:, t * 128:(t + 1) * 128]
                    cnt = rt if cnt is None else cnt + rt
                part = jnp.dot(r.astype(BF16), xv[k0:k0 + KC, :], preferred_element_type=F32)
                acc = part if acc is None else acc + part
            for c in range(4):
                s_ref[r4 * 4 + c] = acc[:, c * 128:(c + 1) * 128].reshape(4, 4, 4, 8, 128)
            cb = jnp.broadcast_to(jnp.sum(cnt, axis=1, keepdims=True), (512, 128)).reshape(64, 8, 128)
            cb = jnp.where((lane >= 32 * r4) & (lane < 32 * r4 + 32), cb, 0.0)
            s_ref[16] = s_ref[16] + cb.reshape(4, 4, 4, 8, 128)

        for k in range(3):
            reduce_phase(k)

        at = (me["z"], me["y"], me["x"])
        ntile = s_ref[(16,) + at]
        vals, tile = [], jnp.zeros((8, 128), F32)
        for r4 in range(4):
            n = jnp.broadcast_to(ntile[:, 32 * r4:32 * r4 + 1], (8, 128))
            row = [s_ref[(r4 * 4 + c,) + at] / (n + COUNT_EPS) for c in range(4)]
            vals.append(row)
            sq = (row[0] * row[0] + row[1] * row[1]) + (row[2] * row[2] + row[3] * row[3])
            hh = jnp.broadcast_to(0.5 * jnp.sum(sq, axis=1, keepdims=True), (8, 128))
            lw = jnp.log((n + PRIOR_ALPHA) / (n_total + k_total * PRIOR_ALPHA))
            tile = jnp.where(lax.div(lane, 16) == r4, hh, tile)
            tile = jnp.where(lax.div(lane, 16) == 4 + r4, lw, tile)

        @pl.when(sweep < sweeps - 1)
        def _():
            for r2 in range(2):
                for c in range(4):
                    mu[(r2 * 4 + c,) + at] = cat([vals[2 * r2][c], vals[2 * r2 + 1][c]], 0).astype(BF16)
            ct[at] = tile
            blocks = [[(mu, BF_TILES[0])], [(mu, BF_TILES[1])], [(mu, BF_TILES[2]), (ct, None)]]
            for k in (2, 1, 0):
                gather_phase(k, blocks)

        @pl.when(sweep == sweeps - 1)
        def _():
            for r4 in range(4):
                for c in range(4):
                    muf[(r4 * 4 + c,) + at] = vals[r4][c]
            muf[(16,) + at] = tile
            blocks = [[(muf, SUM_TILES[p])] for p in range(3)]
            for k in (2, 1, 0):
                gather_phase(k, blocks)

    o0 = pltpu.make_async_copy(muf.at[pl.ds(0, 16)], out_mu, load_sem.at[0])
    o1 = pltpu.make_async_copy(muf.at[16], out_ct, load_sem.at[1])
    o0.start()
    o1.start()
    o0.wait()
    o1.wait()


def solution(mesh):
    row_groups = mesh.shape["pts"]
    comp_groups = mesh.shape["comp"]

    def per_device(points, mean_vecs, log_w, inv_temp):
        n_pts = points.shape[0]
        n_total = n_pts * row_groups
        k_total = mean_vecs.shape[0] * comp_groups
        sweeps = inv_temp.shape[0]
        mu_in = mean_vecs.astype(BF16).reshape(64, 2, 16, 4, 128).transpose(1, 3, 0, 2, 4)
        mu_in = mu_in.reshape(8, 4, 4, 4, 16, 128)
        sq = 0.5 * jnp.sum(mean_vecs * mean_vecs, axis=1)
        both = cat([v.reshape(64, 4, 8).transpose(0, 2, 1) for v in (sq, log_w)], 2)
        ct_in = jnp.broadcast_to(both[..., None], (64, 8, 8, 16)).reshape(4, 4, 4, 8, 128)

        def rbuf(k):
            shapes = []
            for (lo, hi), order in zip(SUM_TILES, ORDERS):
                if k == 2:
                    shapes.append(pltpu.VMEM((3, hi - lo, 8, 128), F32))
                    continue
                dims = [2 if d == order[2] else 4 for d in ("z", "y", "x") if d not in order[:k + 1]]
                shapes.append(pltpu.VMEM((6, hi - lo, *dims, 8, 128), F32))
            return shapes

        any_spec = pl.BlockSpec(memory_space=pl.ANY)
        out_mu, out_ct, out_lse = pl.pallas_call(
            functools.partial(kernel, n_total, k_total, sweeps),
            out_shape=(jax.ShapeDtypeStruct((16, 4, 4, 4, 8, 128), F32),
                       jax.ShapeDtypeStruct((4, 4, 4, 8, 128), F32),
                       jax.ShapeDtypeStruct((1, n_pts), F32)),
            in_specs=[any_spec, any_spec, any_spec, pl.BlockSpec(memory_space=pltpu.SMEM)],
            out_specs=(any_spec, any_spec, pl.BlockSpec(memory_space=pltpu.VMEM)),
            scratch_shapes=[
                pltpu.VMEM((n_pts, 512), BF16),
                pltpu.VMEM((4, 512, n_pts), F32),
                pltpu.VMEM((4, 512, PB), F32),
                pltpu.VMEM((4, 512, PB), F32),
                pltpu.VMEM((17, 4, 4, 4, 8, 128), F32),
                pltpu.VMEM((17, 4, 4, 4, 8, 128), F32),
                pltpu.VMEM((8, 4, 4, 4, 16, 128), BF16),
                pltpu.VMEM((4, 4, 4, 8, 128), F32),
                pltpu.VMEM((4, 512, 128), F32),
                pltpu.VMEM((4, 512, 128), F32),
                pltpu.VMEM((8, n_pts), F32),
                pltpu.VMEM((2, 8, n_pts), F32),
                pltpu.VMEM((1, n_pts), F32),
                pltpu.VMEM((1, n_pts), F32),
                *rbuf(0), *rbuf(1), *rbuf(2),
                pltpu.SemaphoreType.DMA((3,)),
                pltpu.SemaphoreType.DMA,
                pltpu.SemaphoreType.DMA((2,)),
                pltpu.SemaphoreType.DMA((3, 3, 6)),
                pltpu.SemaphoreType.DMA((3, 3, 6)),
                pltpu.SemaphoreType.DMA((3, 2, 3, 6)),
                pltpu.SemaphoreType.DMA((3, 2, 3, 6)),
            ],
            compiler_params=pltpu.CompilerParams(has_side_effects=True, vmem_limit_bytes=67043328),
            cost_estimate=pl.CostEstimate(flops=6 * 2 * n_pts * 2048 * 512, bytes_accessed=1 << 24, transcendentals=0),
        )(points, mu_in, ct_in, inv_temp)
        means = out_mu.reshape(4, 4, 64, 8, 128).transpose(2, 0, 3, 1, 4).reshape(2048, 512)
        logw = out_ct.reshape(64, 8, 8, 16)[:, :, 4:, 0].transpose(0, 2, 1).reshape(2048)
        return means, logw, out_lse.reshape(n_pts)

    row_spec = P(("fit", "pts"))
    comp_spec = P(("fit", "comp"))
    return jax.shard_map(
        per_device,
        mesh=mesh,
        in_specs=(P(("fit", "pts"), None), P(("fit", "comp"), None), comp_spec, P()),
        out_specs=(P(("fit", "comp"), None), comp_spec, row_spec),
        check_vma=False,
    )
```

```python
import functools
import math

import jax
import jax.numpy as jnp
from jax import lax
from jax.experimental import pallas as pl
from jax.experimental.pallas import tpu as pltpu
from jax.sharding import PartitionSpec as P

PRIOR_ALPHA = 1e-3
COUNT_EPS = 1e-6
LOG2E = math.log2(math.e)
LN2 = math.log(2.0)
F32, BF16 = jnp.float32, jnp.bfloat16
MESH = pl.DeviceIdType.MESH

DIMS = ("z", "y", "x")
ORDERS = (("x", "y", "z"), ("y", "z", "x"), ("z", "x", "y"))
SUM_TILES = ((0, 3), (3, 6), (6, 9))
BF_TILES = (((0, 2), (2, 3), (3, 4)), ((0, 1), (1, 2), (2, 4)))
PB = 512
KC = 512


def cat(parts, axis):
    return jnp.concatenate(parts, axis=axis)


def kernel(n_total, k_total, sweeps, x_hbm, mean_hbm, lw_ref, beta_ref, out_mu, out_lw, out_lse,
           xv, e_ref, l0, l1, s_ref, muf, mu, ct, hrep, lrep, st, stp, wrow, qh,
           ra0, ra1, ra2, rb0, rb1, rb2, rc0, rc1, rc2,
           load_sem, ex_send, ex_recv, rs_send, rs_recv, ag_send, ag_recv):
    n_pts = xv.shape[0]
    nb = n_pts // PB
    fit, comp, pts = lax.axis_index("fit"), lax.axis_index("comp"), lax.axis_index("pts")
    me = {"z": lax.div(pts, 16), "y": lax.rem(lax.div(pts, 4), 4), "x": lax.rem(pts, 4)}
    near = {r: {d: lax.rem(me[d] + r, 4) for d in DIMS} for r in (1, 2, 3)}
    bufs = ((ra0, ra1, ra2), (rb0, rb1, rb2), (rc0, rc1, rc2))
    own = (me["z"], me["y"], me["x"])
    lane = lax.broadcasted_iota(jnp.int32, (8, 128), 1)

    def dev(d, r):
        c = {**me, d: near[r][d]}
        return (fit, comp, c["z"] * 16 + c["y"] * 4 + c["x"])

    def coord(d, r):
        return near[r][d] if r else me[d]

    def place(p, k, r, half=None):
        order = ORDERS[p]
        sel = {order[j]: me[order[j]] for j in range(k)}
        sel[order[k]] = coord(order[k], r)
        if half is not None:
            sel[order[2]] = pl.ds(2 * half, 2)
        return tuple(sel.get(d, slice(None)) for d in DIMS)

    def remote(src, dst, ss, rs, device):
        return pltpu.make_async_remote_copy(src_ref=src, dst_ref=dst, send_sem=ss, recv_sem=rs,
                                            device_id=device, device_id_type=MESH)

    def sums(h, p):
        return (h, pl.ds(SUM_TILES[p][0], SUM_TILES[p][1] - SUM_TILES[p][0]))

    def rs_copy(h, p, k, i):
        d, buf = ORDERS[p][k], bufs[k][p]
        if k == 2:
            r = (1, 3, 2)[i]
            src = s_ref.at[sums(h, p) + place(p, k, r)]
        else:
            r = (1, 3, 1, 1, 3, 3)[i]
            if i in (2, 5):
                src = buf.at[h, 0 if i == 2 else 1]
            else:
                to, half = {0: (2, 0), 1: (2, 1), 3: (1, 1), 4: (3, 0)}[i]
                src = s_ref.at[sums(h, p) + place(p, k, to, half)]
        j = 6 * k + i
        return remote(src, buf.at[h, i], rs_send.at[h, p, j], rs_recv.at[h, p, j], dev(d, r))

    def rs_start(h, k):
        for i in ((2, 0, 1) if k == 2 else (0, 1, 3, 4)):
            for p in range(3):
                rs_copy(h, p, k, i).start()

    def rs_relay(h, k):
        for p in range(3):
            buf = bufs[k][p]
            for i, to, half, nxt in ((0, 1, 0, 2), (1, 3, 1, 5)):
                rs_copy(h, p, k, i).wait_recv()
                buf[h, i] = buf[h, i] + s_ref[sums(h, p) + place(p, k, to, half)]
                rs_copy(h, p, k, nxt).start()

    def rs_finish(h, k):
        for p in range(3):
            buf = bufs[k][p]
            if k == 2:
                for i in range(3):
                    rs_copy(h, p, k, i).wait()
                mine = sums(h, p) + own
                s_ref[mine] = (s_ref[mine] + buf[h, 0]) + (buf[h, 1] + buf[h, 2])
                continue
            for half, i, j in ((0, 2, 4), (1, 3, 5)):
                rs_copy(h, p, k, i).wait_recv()
                rs_copy(h, p, k, j).wait_recv()
                mine = sums(h, p) + place(p, k, 0, half)
                s_ref[mine] = s_ref[mine] + (buf[h, i] + buf[h, j])
            for i in range(6):
                rs_copy(h, p, k, i).wait_send()

    def bf_units(h):
        units = []
        for p, (lo, hi) in enumerate(BF_TILES[h]):
            units.append((mu, (h, pl.ds(lo, hi - lo)), p))
        return units + [(ct, (h,), 1)]

    def f32_units(h):
        return [(muf, sums(h, p), p) for p in range(3)]

    def ag_copy(units, h, u, k, i):
        ref, lead, p = units[u]
        d = ORDERS[p][k]
        if k == 2:
            r = (1, 3, 2)[i]
            view = ref.at[lead + place(p, k, 0)]
        else:
            frm, half, r = ((0, 0, 1), (0, 1, 3), (0, 1, 1), (0, 0, 3), (3, 0, 1), (1, 1, 3))[i]
            view = ref.at[lead + place(p, k, frm, half)]
        j = 6 * k + i
        return remote(view, view, ag_send.at[h, u, j], ag_recv.at[h, u, j], dev(d, r))

    def ag_start(units, h, k):
        for i in ((2, 0, 1) if k == 2 else range(4)):
            for u in range(len(units)):
                ag_copy(units, h, u, k, i).start()

    def ag_relay(units, h, k):
        for u in range(len(units)):
            for i, nxt in ((0, 4), (1, 5)):
                ag_copy(units, h, u, k, i).wait_recv()
                ag_copy(units, h, u, k, nxt).start()

    def ag_finish(units, h, k):
        for u in range(len(units)):
            if k == 2:
                for i in range(3):
                    ag_copy(units, h, u, k, i).wait()
                continue
            for i in range(2, 6):
                ag_copy(units, h, u, k, i).wait_recv()
            for i in range(6):
                ag_copy(units, h, u, k, i).wait_send()

    def column(v, lanes):
        return jnp.broadcast_to(v[:, lanes:lanes + 1], (v.shape[0], 128))

    def expand(h):
        t = ct[h].reshape(512, 128)
        for hh in range(2):
            hrep[h, hh] = column(t, 32 * hh)
            lrep[h, hh] = column(t, 64 + 32 * hh) * LOG2E

    def logits(h, j, lref, b2):
        cols = pl.ds(pl.multiple_of(j * PB, PB), PB)
        xj = xv[cols, :]
        q = qh[:, cols]
        rows = cat([mu[h, c].reshape(1024, 128) for c in range(4)], 1)
        a = lax.dot_general(rows, xj, (((1,), (1,)), ((), ())), preferred_element_type=F32)
        a = a.reshape(64, 2, 8, PB)
        top = None
        for hh in range(2):
            hc = cat([hrep[h, hh]] * (PB // 128), 1)
            lc = cat([lrep[h, hh]] * (PB // 128), 1)
            v = ((a[:, hh].reshape(512, PB) - hc) - q) * b2 + lc
            lref[hh] = v
            t = jnp.max(v.reshape(64, 8, PB), axis=0)
            top = t if top is None else jnp.maximum(top, t)
        st[2 * h, :, cols] = jnp.max(top, axis=0, keepdims=True)

    def exps(h, j, lref):
        cols = pl.ds(pl.multiple_of(j * PB, PB), PB)
        m = st[2 * h, :, cols]
        tot = None
        for hh in range(2):
            e = jnp.exp2(lref[hh] - m)
            e_ref[2 * h + hh, :, cols] = e
            t = jnp.sum(e.reshape(64, 8, PB), axis=0)
            tot = t if tot is None else tot + t
        st[2 * h + 1, :, cols] = jnp.sum(tot, axis=0, keepdims=True)

    def scores(h, b2, during=()):
        logits(h, 0, l0, b2)

        @pl.loop(0, nb // 2 - 1)
        def _(i):
            for n, step in enumerate(during):
                pl.when(i == n)(step)
            logits(h, 2 * i + 1, l1, b2)
            exps(h, 2 * i, l0)
            logits(h, 2 * i + 2, l0, b2)
            exps(h, 2 * i + 1, l1)

        logits(h, nb - 1, l1, b2)
        exps(h, nb - 2, l0)
        exps(h, nb - 1, l1)

    def normalise(slot):
        ex = remote(st, stp.at[slot], ex_send, ex_recv.at[slot], (fit, 1 - comp, pts))
        ex.start()
        for h in range(2):
            s_ref[h, 8] = jnp.zeros((4, 4, 4, 8, 128), F32)
        ex.wait()
        tops = [st[0], st[2], stp[slot, 0], stp[slot, 2]]
        mm = jnp.maximum(jnp.maximum(tops[0], tops[1]), jnp.maximum(tops[2], tops[3]))
        tot = (st[1] * jnp.exp2(tops[0] - mm) + st[3] * jnp.exp2(tops[1] - mm)) + (
            stp[slot, 1] * jnp.exp2(tops[2] - mm) + stp[slot, 3] * jnp.exp2(tops[3] - mm))
        lse2 = mm + jnp.log2(tot)
        for h in range(2):
            wrow[h] = jnp.exp2(tops[h] - lse2)
        return lse2

    def moments():
        @pl.loop(0, 4)
        def _(r4):
            h, hh = lax.div(r4, 2), lax.rem(r4, 2)
            pl.when(r4 == 2)(lambda: rs_start(0, 0))
            pl.when(r4 == 3)(lambda: rs_relay(0, 0))
            acc, cnt = None, None
            for kc in range(n_pts // KC):
                k0 = kc * KC
                r = e_ref[r4, :, k0:k0 + KC] * wrow[h, :, k0:k0 + KC]
                for t in range(KC // 128):
                    rt = r[:, t * 128:(t + 1) * 128]
                    cnt = rt if cnt is None else cnt + rt
                part = jnp.dot(r.astype(BF16), xv[k0:k0 + KC, :], preferred_element_type=F32)
                acc = part if acc is None else acc + part
            for c in range(4):
                s_ref[h, hh * 4 + c] = acc[:, c * 128:(c + 1) * 128].reshape(4, 4, 4, 8, 128)
            cb = jnp.broadcast_to(jnp.sum(cnt, axis=1, keepdims=True), (512, 128)).reshape(64, 8, 128)
            cb = jnp.where(lax.div(lane, 64) == hh, cb, 0.0)
            s_ref[h, 8] = s_ref[h, 8] + cb.reshape(4, 4, 4, 8, 128)

    def update(h):
        ntile = s_ref[(h, 8) + own]
        vals, tile = [], jnp.zeros((8, 128), F32)
        for hh in range(2):
            n = column(ntile, 64 * hh)
            row = [s_ref[(h, hh * 4 + c) + own] / (n + COUNT_EPS) for c in range(4)]
            vals.append(row)
            sq = (row[0] * row[0] + row[1] * row[1]) + (row[2] * row[2] + row[3] * row[3])
            hc = jnp.broadcast_to(0.5 * jnp.sum(sq, axis=1, keepdims=True), (8, 128))
            lw = jnp.log((n + PRIOR_ALPHA) / (n_total + k_total * PRIOR_ALPHA))
            tile = jnp.where(lax.div(lane, 32) == hh, hc, tile)
            tile = jnp.where(lax.div(lane, 32) == 2 + hh, lw, tile)
        return vals, tile

    def update_bf(h):
        vals, tile = update(h)
        for c in range(4):
            mu[(h, c) + own] = cat([vals[0][c], vals[1][c]], 0).astype(BF16)
        ct[(h,) + own] = tile

    def update_f32(h):
        vals, tile = update(h)
        for hh in range(2):
            for c in range(4):
                muf[(h, hh * 4 + c) + own] = vals[hh][c]
        muf[(h, 8) + own] = tile

    def exchange(units, upd):
        u0, u1 = units
        rs_start(1, 0)
        rs_finish(0, 0)
        rs_start(0, 1)
        rs_relay(1, 0)
        rs_relay(0, 1)
        rs_finish(0, 1)
        rs_start(0, 2)
        rs_finish(1, 0)
        rs_start(1, 1)
        rs_finish(0, 2)
        upd(0)
        ag_start(u0, 0, 2)
        rs_relay(1, 1)
        ag_finish(u0, 0, 2)
        ag_start(u0, 0, 1)
        rs_finish(1, 1)
        rs_start(1, 2)
        ag_relay(u0, 0, 1)
        ag_finish(u0, 0, 1)
        ag_start(u0, 0, 0)
        rs_finish(1, 2)
        upd(1)
        ag_start(u1, 1, 2)
        ag_relay(u0, 0, 0)
        ag_finish(u1, 1, 2)
        ag_start(u1, 1, 1)
        ag_finish(u0, 0, 0)

    loads = [pltpu.make_async_copy(x_hbm, xv, load_sem.at[16])]
    for h in range(2):
        for hh in range(2):
            for c in range(4):
                t = hh * 4 + c
                loads.append(pltpu.make_async_copy(
                    mean_hbm.at[:, :, :, h, hh, :, pl.ds(c * 128, 128)], s_ref.at[h, t], load_sem.at[8 * h + t]))
    for c in loads[1:] + loads[:1]:
        c.start()
    for c in loads[1:]:
        c.wait()
    st[...] = jnp.zeros_like(st)

    @pl.loop(0, 2)
    def _(h):
        for hh in range(2):
            v = [s_ref[h, hh * 4 + c].reshape(512, 128) for c in range(4)]
            sq = (v[0] * v[0] + v[1] * v[1]) + (v[2] * v[2] + v[3] * v[3])
            hrep[h, hh] = jnp.broadcast_to(0.5 * jnp.sum(sq, axis=1, keepdims=True), (512, 128))
        for c in range(4):
            v = cat([s_ref[h, c].reshape(64, 8, 128), s_ref[h, 4 + c].reshape(64, 8, 128)], 1)
            mu[h, c] = v.astype(BF16).reshape(4, 4, 4, 16, 128)

    for i in range(16):
        col = jnp.broadcast_to(lw_ref[i:i + 1, :] * LOG2E, (128, 128)).T
        for g in range(4):
            for r4 in range(4):
                lo = 32 * g + 8 * r4
                lrep[r4 // 2, r4 % 2, (4 * i + g) * 8:(4 * i + g) * 8 + 8, :] = col[lo:lo + 8, :]
    loads[0].wait()

    @pl.loop(0, n_pts // 128)
    def _(i):
        rows = pl.ds(pl.multiple_of(i * 128, 128), 128)
        xb = xv[rows, :].astype(F32)
        sq = xb * xb
        sq = (sq[:, 0:128] + sq[:, 128:256]) + (sq[:, 256:384] + sq[:, 384:512])
        qh[:, rows] = jnp.sum(sq.T, axis=0, keepdims=True) * 0.5

    @pl.loop(0, 2)
    def _(h):
        scores(h, beta_ref[0] * (2.0 * LOG2E))

    bf = (bf_units(0), bf_units(1))

    @pl.loop(0, sweeps - 1)
    def _(sweep):
        b2 = beta_ref[sweep + 1] * (2.0 * LOG2E)
        normalise(lax.rem(sweep, 2))
        moments()
        exchange(bf, update_bf)
        expand(0)

        def next_phase():
            ag_finish(bf[1], 1, 1)
            ag_start(bf[1], 1, 0)

        scores(0, b2, (lambda: ag_relay(bf[1], 1, 1), next_phase, lambda: ag_relay(bf[1], 1, 0)))
        ag_finish(bf[1], 1, 0)
        expand(1)
        scores(1, b2)

    out_lse[...] = normalise((sweeps - 1) % 2) * LN2
    moments()
    f32 = (f32_units(0), f32_units(1))
    exchange(f32, update_f32)
    stores = []
    for h in range(2):
        if h == 1:
            ag_relay(f32[1], 1, 1)
        for hh in range(2):
            for c in range(4):
                t = hh * 4 + c
                stores.append(pltpu.make_async_copy(
                    muf.at[h, t], out_mu.at[:, :, :, h, hh, :, pl.ds(c * 128, 128)], load_sem.at[8 * h + t]))
                if h == 0:
                    stores[-1].start()
    ag_finish(f32[1], 1, 1)
    ag_start(f32[1], 1, 0)
    ag_relay(f32[1], 1, 0)
    ag_finish(f32[1], 1, 0)
    for c in stores[8:]:
        c.start()
    for i in range(16):
        tiles = []
        for g in range(4):
            for r4 in range(4):
                tiles.append(column(muf[r4 // 2, 8, i // 4, i % 4, g], 64 + 32 * (r4 % 2)))
        out_lw[i:i + 1, :] = cat(tiles, 0).T[0:1, :]
    for c in stores:
        c.wait()


def solution(mesh):
    row_groups = mesh.shape["pts"]
    comp_groups = mesh.shape["comp"]

    def per_device(points, mean_vecs, log_w, inv_temp):
        n_pts = points.shape[0]
        n_total = n_pts * row_groups
        k_total = mean_vecs.shape[0] * comp_groups
        sweeps = inv_temp.shape[0]

        def rbuf(k):
            shapes = []
            for (lo, hi), order in zip(SUM_TILES, ORDERS):
                if k == 2:
                    shapes.append(pltpu.VMEM((2, 3, hi - lo, 8, 128), F32))
                    continue
                dims = [2 if d == order[2] else 4 for d in DIMS if d not in order[:k + 1]]
                shapes.append(pltpu.VMEM((2, 6, hi - lo, *dims, 8, 128), F32))
            return shapes

        any_spec = pl.BlockSpec(memory_space=pl.ANY)
        vmem_spec = pl.BlockSpec(memory_space=pltpu.VMEM)
        out_mu, out_lw, out_lse = pl.pallas_call(
            functools.partial(kernel, n_total, k_total, sweeps),
            out_shape=(jax.ShapeDtypeStruct((4, 4, 4, 2, 2, 8, 512), F32),
                       jax.ShapeDtypeStruct((16, 128), F32),
                       jax.ShapeDtypeStruct((1, n_pts), F32)),
            in_specs=[any_spec, any_spec, vmem_spec, pl.BlockSpec(memory_space=pltpu.SMEM)],
            out_specs=(any_spec, vmem_spec, vmem_spec),
            scratch_shapes=[
                pltpu.VMEM((n_pts, 512), BF16),
                pltpu.VMEM((4, 512, n_pts), F32),
                pltpu.VMEM((2, 512, PB), F32),
                pltpu.VMEM((2, 512, PB), F32),
                pltpu.VMEM((2, 9, 4, 4, 4, 8, 128), F32),
                pltpu.VMEM((2, 9, 4, 4, 4, 8, 128), F32),
                pltpu.VMEM((2, 4, 4, 4, 4, 16, 128), BF16),
                pltpu.VMEM((2, 4, 4, 4, 8, 128), F32),
                pltpu.VMEM((2, 2, 512, 128), F32),
                pltpu.VMEM((2, 2, 512, 128), F32),
                pltpu.VMEM((4, 1, n_pts), F32),
                pltpu.VMEM((2, 4, 1, n_pts), F32),
                pltpu.VMEM((2, 1, n_pts), F32),
                pltpu.VMEM((1, n_pts), F32),
                *rbuf(0), *rbuf(1), *rbuf(2),
                pltpu.SemaphoreType.DMA((17,)),
                pltpu.SemaphoreType.DMA,
                pltpu.SemaphoreType.DMA((2,)),
                pltpu.SemaphoreType.DMA((2, 3, 15)),
                pltpu.SemaphoreType.DMA((2, 3, 15)),
                pltpu.SemaphoreType.DMA((2, 4, 15)),
                pltpu.SemaphoreType.DMA((2, 4, 15)),
            ],
            compiler_params=pltpu.CompilerParams(has_side_effects=True, vmem_limit_bytes=67043328),
            cost_estimate=pl.CostEstimate(flops=6 * 2 * n_pts * 2048 * 512, bytes_accessed=1 << 24, transcendentals=0),
        )(points, mean_vecs.reshape(4, 4, 4, 2, 2, 8, 512), log_w.reshape(16, 128), inv_temp)
        return out_mu.reshape(2048, 512), out_lw.reshape(2048), out_lse.reshape(n_pts)

    row_spec = P(("fit", "pts"))
    comp_spec = P(("fit", "comp"))
    return jax.shard_map(
        per_device,
        mesh=mesh,
        in_specs=(P(("fit", "pts"), None), P(("fit", "comp"), None), comp_spec, P()),
        out_specs=(P(("fit", "comp"), None), comp_spec, row_spec),
        check_vma=False,
    )
```

```python
import functools
import math

import jax
import jax.numpy as jnp
from jax import lax
from jax.experimental import pallas as pl
from jax.experimental.pallas import tpu as pltpu
from jax.sharding import PartitionSpec as P

PRIOR_ALPHA = 1e-3
COUNT_EPS = 1e-6
LOG2E = math.log2(math.e)
LN2 = math.log(2.0)
F32, BF16 = jnp.float32, jnp.bfloat16
MESH = pl.DeviceIdType.MESH

DIMS = ("z", "y", "x")
ORDERS = (("x", "y", "z"), ("y", "z", "x"), ("z", "x", "y"))
SUM_TILES = ((0, 3), (3, 6), (6, 9))
BF_TILES = (((0, 2), (2, 3), (3, 4)), ((0, 1), (1, 2), (2, 4)))
PB = 512
KC = 512


def cat(parts, axis):
    return jnp.concatenate(parts, axis=axis)


def kernel(n_total, k_total, sweeps, x_hbm, mean_hbm, lw_ref, beta_ref, out_mu, out_lw, out_lse,
           xv, e_ref, l0, l1, s_ref, muf, mu, ct, hrep, lrep, st, stp, wrow, qh,
           ra0, ra1, ra2, rb0, rb1, rb2, rc0, rc1, rc2,
           load_sem, ex_send, ex_recv, rs_send, rs_recv, ag_send, ag_recv):
    n_pts = xv.shape[0]
    nb = n_pts // PB
    fit, comp, pts = lax.axis_index("fit"), lax.axis_index("comp"), lax.axis_index("pts")
    me = {"z": lax.div(pts, 16), "y": lax.rem(lax.div(pts, 4), 4), "x": lax.rem(pts, 4)}
    near = {r: {d: lax.rem(me[d] + r, 4) for d in DIMS} for r in (1, 2, 3)}
    bufs = ((ra0, ra1, ra2), (rb0, rb1, rb2), (rc0, rc1, rc2))
    own = (me["z"], me["y"], me["x"])
    lane = lax.broadcasted_iota(jnp.int32, (8, 128), 1)

    def dev(d, r):
        c = {**me, d: near[r][d]}
        return (fit, comp, c["z"] * 16 + c["y"] * 4 + c["x"])

    def coord(d, r):
        return near[r][d] if r else me[d]

    def place(p, k, r, half=None):
        order = ORDERS[p]
        sel = {order[j]: me[order[j]] for j in range(k)}
        sel[order[k]] = coord(order[k], r)
        if half is not None:
            sel[order[2]] = pl.ds(2 * half, 2)
        return tuple(sel.get(d, slice(None)) for d in DIMS)

    def remote(src, dst, ss, rs, device):
        return pltpu.make_async_remote_copy(src_ref=src, dst_ref=dst, send_sem=ss, recv_sem=rs,
                                            device_id=device, device_id_type=MESH)

    def sums(h, p):
        return (h, pl.ds(SUM_TILES[p][0], SUM_TILES[p][1] - SUM_TILES[p][0]))

    def rs_copy(h, p, k, i):
        d, buf = ORDERS[p][k], bufs[k][p]
        if k == 2:
            r = (1, 3, 2)[i]
            src = s_ref.at[sums(h, p) + place(p, k, r)]
        else:
            r = (1, 3, 1, 1, 3, 3)[i]
            if i in (2, 5):
                src = buf.at[h, 0 if i == 2 else 1]
            else:
                to, half = {0: (2, 0), 1: (2, 1), 3: (1, 1), 4: (3, 0)}[i]
                src = s_ref.at[sums(h, p) + place(p, k, to, half)]
        j = 6 * k + i
        return remote(src, buf.at[h, i], rs_send.at[h, p, j], rs_recv.at[h, p, j], dev(d, r))

    def rs_start(h, k):
        for i in ((2, 0, 1) if k == 2 else (0, 1, 3, 4)):
            for p in range(3):
                rs_copy(h, p, k, i).start()

    def rs_relay(h, k):
        for p in range(3):
            buf = bufs[k][p]
            for i, to, half, nxt in ((0, 1, 0, 2), (1, 3, 1, 5)):
                rs_copy(h, p, k, i).wait_recv()
                buf[h, i] = buf[h, i] + s_ref[sums(h, p) + place(p, k, to, half)]
                rs_copy(h, p, k, nxt).start()

    def rs_finish(h, k):
        for p in range(3):
            buf = bufs[k][p]
            if k == 2:
                for i in range(3):
                    rs_copy(h, p, k, i).wait()
                mine = sums(h, p) + own
                s_ref[mine] = (s_ref[mine] + buf[h, 0]) + (buf[h, 1] + buf[h, 2])
                continue
            for half, i, j in ((0, 2, 4), (1, 3, 5)):
                rs_copy(h, p, k, i).wait_recv()
                rs_copy(h, p, k, j).wait_recv()
                mine = sums(h, p) + place(p, k, 0, half)
                s_ref[mine] = s_ref[mine] + (buf[h, i] + buf[h, j])
            for i in range(6):
                rs_copy(h, p, k, i).wait_send()

    def bf_units(h):
        units = []
        for p, (lo, hi) in enumerate(BF_TILES[h]):
            units.append((mu, (h, pl.ds(lo, hi - lo)), p))
        return units + [(ct, (h,), 1)]

    def f32_units(h):
        return [(muf, sums(h, p), p) for p in range(3)]

    def ag_copy(units, h, u, k, i):
        ref, lead, p = units[u]
        d = ORDERS[p][k]
        if k == 2:
            r = (1, 3, 2)[i]
            view = ref.at[lead + place(p, k, 0)]
        else:
            frm, half, r = ((0, 0, 1), (0, 1, 3), (0, 1, 1), (0, 0, 3), (3, 0, 1), (1, 1, 3))[i]
            view = ref.at[lead + place(p, k, frm, half)]
        j = 6 * k + i
        return remote(view, view, ag_send.at[h, u, j], ag_recv.at[h, u, j], dev(d, r))

    def ag_start(units, h, k):
        for i in ((2, 0, 1) if k == 2 else range(4)):
            for u in range(len(units)):
                ag_copy(units, h, u, k, i).start()

    def ag_relay(units, h, k):
        for u in range(len(units)):
            for i, nxt in ((0, 4), (1, 5)):
                ag_copy(units, h, u, k, i).wait_recv()
                ag_copy(units, h, u, k, nxt).start()

    def ag_finish(units, h, k):
        for u in range(len(units)):
            if k == 2:
                for i in range(3):
                    ag_copy(units, h, u, k, i).wait()
                continue
            for i in range(2, 6):
                ag_copy(units, h, u, k, i).wait_recv()
            for i in range(6):
                ag_copy(units, h, u, k, i).wait_send()

    def column(v, lanes):
        return jnp.broadcast_to(v[:, lanes:lanes + 1], (v.shape[0], 128))

    def expand(h):
        t = ct[h].reshape(512, 128)
        for hh in range(2):
            hrep[h, hh] = column(t, 32 * hh)
            lrep[h, hh] = column(t, 64 + 32 * hh) * LOG2E

    def logits(h, j, lref, b2):
        cols = pl.ds(pl.multiple_of(j * PB, PB), PB)
        xj = xv[cols, :]
        q = qh[:, cols]
        rows = cat([mu[h, c].reshape(1024, 128) for c in range(4)], 1)
        a = lax.dot_general(rows, xj, (((1,), (1,)), ((), ())), preferred_element_type=F32)
        a = a.reshape(64, 2, 8, PB)
        top = None
        for hh in range(2):
            hc = cat([hrep[h, hh]] * (PB // 128), 1)
            lc = cat([lrep[h, hh]] * (PB // 128), 1)
            v = ((a[:, hh].reshape(512, PB) - hc) - q) * b2 + lc
            lref[hh] = v
            t = jnp.max(v.reshape(64, 8, PB), axis=0)
            top = t if top is None else jnp.maximum(top, t)
        st[2 * h, :, cols] = jnp.max(top, axis=0, keepdims=True)

    def exps(h, j, lref):
        cols = pl.ds(pl.multiple_of(j * PB, PB), PB)
        m = st[2 * h, :, cols]
        tot = None
        for hh in range(2):
            e = jnp.exp2(lref[hh] - m)
            e_ref[2 * h + hh, :, cols] = e
            t = jnp.sum(e.reshape(64, 8, PB), axis=0)
            tot = t if tot is None else tot + t
        st[2 * h + 1, :, cols] = jnp.sum(tot, axis=0, keepdims=True)

    def scores(h, b2, during=()):
        logits(h, 0, l0, b2)

        @pl.loop(0, nb // 2 - 1)
        def _(i):
            for n, step in enumerate(during):
                pl.when(i == n)(step)
            logits(h, 2 * i + 1, l1, b2)
            exps(h, 2 * i, l0)
            logits(h, 2 * i + 2, l0, b2)
            exps(h, 2 * i + 1, l1)

        logits(h, nb - 1, l1, b2)
        exps(h, nb - 2, l0)
        exps(h, nb - 1, l1)

    def normalise(slot):
        ex = remote(st, stp.at[slot], ex_send, ex_recv.at[slot], (fit, 1 - comp, pts))
        ex.start()
        for h in range(2):
            s_ref[h, 8] = jnp.zeros((4, 4, 4, 8, 128), F32)
        ex.wait()
        tops = [st[0], st[2], stp[slot, 0], stp[slot, 2]]
        mm = jnp.maximum(jnp.maximum(tops[0], tops[1]), jnp.maximum(tops[2], tops[3]))
        tot = (st[1] * jnp.exp2(tops[0] - mm) + st[3] * jnp.exp2(tops[1] - mm)) + (
            stp[slot, 1] * jnp.exp2(tops[2] - mm) + stp[slot, 3] * jnp.exp2(tops[3] - mm))
        lse2 = mm + jnp.log2(tot)
        for h in range(2):
            wrow[h] = jnp.exp2(tops[h] - lse2)
        return lse2

    def moments():
        @pl.loop(0, 4)
        def _(r4):
            h, hh = lax.div(r4, 2), lax.rem(r4, 2)
            pl.when(r4 == 2)(lambda: rs_start(0, 0))
            pl.when(r4 == 3)(lambda: rs_relay(0, 0))
            acc, cnt = None, None
            for kc in range(n_pts // KC):
                k0 = kc * KC
                r = e_ref[r4, :, k0:k0 + KC] * wrow[h, :, k0:k0 + KC]
                for t in range(KC // 128):
                    rt = r[:, t * 128:(t + 1) * 128]
                    cnt = rt if cnt is None else cnt + rt
                part = jnp.dot(r.astype(BF16), xv[k0:k0 + KC, :], preferred_element_type=F32)
                acc = part if acc is None else acc + part
            for c in range(4):
                s_ref[h, hh * 4 + c] = acc[:, c * 128:(c + 1) * 128].reshape(4, 4, 4, 8, 128)
            cb = jnp.broadcast_to(jnp.sum(cnt, axis=1, keepdims=True), (512, 128)).reshape(64, 8, 128)
            cb = jnp.where(lax.div(lane, 64) == hh, cb, 0.0)
            s_ref[h, 8] = s_ref[h, 8] + cb.reshape(4, 4, 4, 8, 128)

    def update(h):
        ntile = s_ref[(h, 8) + own]
        vals, tile = [], jnp.zeros((8, 128), F32)
        for hh in range(2):
            n = column(ntile, 64 * hh)
            row = [s_ref[(h, hh * 4 + c) + own] / (n + COUNT_EPS) for c in range(4)]
            vals.append(row)
            sq = (row[0] * row[0] + row[1] * row[1]) + (row[2] * row[2] + row[3] * row[3])
            hc = jnp.broadcast_to(0.5 * jnp.sum(sq, axis=1, keepdims=True), (8, 128))
            lw = jnp.log((n + PRIOR_ALPHA) / (n_total + k_total * PRIOR_ALPHA))
            tile = jnp.where(lax.div(lane, 32) == hh, hc, tile)
            tile = jnp.where(lax.div(lane, 32) == 2 + hh, lw, tile)
        return vals, tile

    def update_bf(h):
        vals, tile = update(h)
        for c in range(4):
            mu[(h, c) + own] = cat([vals[0][c], vals[1][c]], 0).astype(BF16)
        ct[(h,) + own] = tile

    def update_f32(h):
        vals, tile = update(h)
        for hh in range(2):
            for c in range(4):
                muf[(h, hh * 4 + c) + own] = vals[hh][c]
        muf[(h, 8) + own] = tile

    def exchange(units, upd):
        u0, u1 = units
        rs_start(1, 0)
        rs_finish(0, 0)
        rs_start(0, 1)
        rs_relay(1, 0)
        rs_relay(0, 1)
        rs_finish(0, 1)
        rs_start(0, 2)
        rs_finish(1, 0)
        rs_start(1, 1)
        rs_finish(0, 2)
        upd(0)
        ag_start(u0, 0, 2)
        rs_relay(1, 1)
        ag_finish(u0, 0, 2)
        ag_start(u0, 0, 1)
        rs_finish(1, 1)
        rs_start(1, 2)
        ag_relay(u0, 0, 1)
        ag_finish(u0, 0, 1)
        ag_start(u0, 0, 0)
        rs_finish(1, 2)
        upd(1)
        ag_start(u1, 1, 2)
        ag_relay(u0, 0, 0)
        ag_finish(u1, 1, 2)
        ag_start(u1, 1, 1)
        ag_finish(u0, 0, 0)

    bar = pltpu.get_barrier_semaphore()
    pl.semaphore_signal(bar, inc=1, device_id=(fit, 1 - comp, pts), device_id_type=MESH)
    for d in DIMS:
        for r in (1, 2, 3):
            pl.semaphore_signal(bar, inc=1, device_id=dev(d, r), device_id_type=MESH)

    loads = [pltpu.make_async_copy(x_hbm, xv, load_sem.at[16])]
    for h in range(2):
        for hh in range(2):
            for c in range(4):
                t = hh * 4 + c
                loads.append(pltpu.make_async_copy(
                    mean_hbm.at[:, :, :, h, hh, :, pl.ds(c * 128, 128)], s_ref.at[h, t], load_sem.at[8 * h + t]))
    for c in loads[1:] + loads[:1]:
        c.start()
    for c in loads[1:]:
        c.wait()
    st[...] = jnp.zeros_like(st)

    @pl.loop(0, 2)
    def _(h):
        for hh in range(2):
            v = [s_ref[h, hh * 4 + c].reshape(512, 128) for c in range(4)]
            sq = (v[0] * v[0] + v[1] * v[1]) + (v[2] * v[2] + v[3] * v[3])
            hrep[h, hh] = jnp.broadcast_to(0.5 * jnp.sum(sq, axis=1, keepdims=True), (512, 128))
        for c in range(4):
            v = cat([s_ref[h, c].reshape(64, 8, 128), s_ref[h, 4 + c].reshape(64, 8, 128)], 1)
            mu[h, c] = v.astype(BF16).reshape(4, 4, 4, 16, 128)

    for i in range(16):
        col = jnp.broadcast_to(lw_ref[i:i + 1, :] * LOG2E, (128, 128)).T
        for g in range(4):
            for r4 in range(4):
                lo = 32 * g + 8 * r4
                lrep[r4 // 2, r4 % 2, (4 * i + g) * 8:(4 * i + g) * 8 + 8, :] = col[lo:lo + 8, :]
    loads[0].wait()

    @pl.loop(0, n_pts // 128)
    def _(i):
        rows = pl.ds(pl.multiple_of(i * 128, 128), 128)
        xb = xv[rows, :].astype(F32)
        sq = xb * xb
        sq = (sq[:, 0:128] + sq[:, 128:256]) + (sq[:, 256:384] + sq[:, 384:512])
        qh[:, rows] = jnp.sum(sq.T, axis=0, keepdims=True) * 0.5

    @pl.loop(0, 2)
    def _(h):
        scores(h, beta_ref[0] * (2.0 * LOG2E))

    pl.semaphore_wait(bar, 10)

    bf = (bf_units(0), bf_units(1))

    @pl.loop(0, sweeps - 1)
    def _(sweep):
        b2 = beta_ref[sweep + 1] * (2.0 * LOG2E)
        normalise(lax.rem(sweep, 2))
        moments()
        exchange(bf, update_bf)
        expand(0)

        def next_phase():
            ag_finish(bf[1], 1, 1)
            ag_start(bf[1], 1, 0)

        scores(0, b2, (lambda: ag_relay(bf[1], 1, 1), next_phase, lambda: ag_relay(bf[1], 1, 0)))
        ag_finish(bf[1], 1, 0)
        expand(1)
        scores(1, b2)

    out_lse[...] = normalise((sweeps - 1) % 2) * LN2
    moments()
    f32 = (f32_units(0), f32_units(1))
    exchange(f32, update_f32)
    stores = []
    for h in range(2):
        if h == 1:
            ag_relay(f32[1], 1, 1)
        for hh in range(2):
            for c in range(4):
                t = hh * 4 + c
                stores.append(pltpu.make_async_copy(
                    muf.at[h, t], out_mu.at[:, :, :, h, hh, :, pl.ds(c * 128, 128)], load_sem.at[8 * h + t]))
                if h == 0:
                    stores[-1].start()
    ag_finish(f32[1], 1, 1)
    ag_start(f32[1], 1, 0)
    ag_relay(f32[1], 1, 0)
    ag_finish(f32[1], 1, 0)
    for c in stores[8:]:
        c.start()
    for i in range(16):
        tiles = []
        for g in range(4):
            for r4 in range(4):
                tiles.append(column(muf[r4 // 2, 8, i // 4, i % 4, g], 64 + 32 * (r4 % 2)))
        out_lw[i:i + 1, :] = cat(tiles, 0).T[0:1, :]
    for c in stores:
        c.wait()


def solution(mesh):
    row_groups = mesh.shape["pts"]
    comp_groups = mesh.shape["comp"]

    def per_device(points, mean_vecs, log_w, inv_temp):
        n_pts = points.shape[0]
        n_total = n_pts * row_groups
        k_total = mean_vecs.shape[0] * comp_groups
        sweeps = inv_temp.shape[0]

        def rbuf(k):
            shapes = []
            for (lo, hi), order in zip(SUM_TILES, ORDERS):
                if k == 2:
                    shapes.append(pltpu.VMEM((2, 3, hi - lo, 8, 128), F32))
                    continue
                dims = [2 if d == order[2] else 4 for d in DIMS if d not in order[:k + 1]]
                shapes.append(pltpu.VMEM((2, 6, hi - lo, *dims, 8, 128), F32))
            return shapes

        any_spec = pl.BlockSpec(memory_space=pl.ANY)
        vmem_spec = pl.BlockSpec(memory_space=pltpu.VMEM)
        out_mu, out_lw, out_lse = pl.pallas_call(
            functools.partial(kernel, n_total, k_total, sweeps),
            out_shape=(jax.ShapeDtypeStruct((4, 4, 4, 2, 2, 8, 512), F32),
                       jax.ShapeDtypeStruct((16, 128), F32),
                       jax.ShapeDtypeStruct((1, n_pts), F32)),
            in_specs=[any_spec, any_spec, vmem_spec, pl.BlockSpec(memory_space=pltpu.SMEM)],
            out_specs=(any_spec, vmem_spec, vmem_spec),
            scratch_shapes=[
                pltpu.VMEM((n_pts, 512), BF16),
                pltpu.VMEM((4, 512, n_pts), F32),
                pltpu.VMEM((2, 512, PB), F32),
                pltpu.VMEM((2, 512, PB), F32),
                pltpu.VMEM((2, 9, 4, 4, 4, 8, 128), F32),
                pltpu.VMEM((2, 9, 4, 4, 4, 8, 128), F32),
                pltpu.VMEM((2, 4, 4, 4, 4, 16, 128), BF16),
                pltpu.VMEM((2, 4, 4, 4, 8, 128), F32),
                pltpu.VMEM((2, 2, 512, 128), F32),
                pltpu.VMEM((2, 2, 512, 128), F32),
                pltpu.VMEM((4, 1, n_pts), F32),
                pltpu.VMEM((2, 4, 1, n_pts), F32),
                pltpu.VMEM((2, 1, n_pts), F32),
                pltpu.VMEM((1, n_pts), F32),
                *rbuf(0), *rbuf(1), *rbuf(2),
                pltpu.SemaphoreType.DMA((17,)),
                pltpu.SemaphoreType.DMA,
                pltpu.SemaphoreType.DMA((2,)),
                pltpu.SemaphoreType.DMA((2, 3, 15)),
                pltpu.SemaphoreType.DMA((2, 3, 15)),
                pltpu.SemaphoreType.DMA((2, 4, 15)),
                pltpu.SemaphoreType.DMA((2, 4, 15)),
            ],
            compiler_params=pltpu.CompilerParams(has_side_effects=True, collective_id=0, vmem_limit_bytes=67043328),
            cost_estimate=pl.CostEstimate(flops=6 * 2 * n_pts * 2048 * 512, bytes_accessed=1 << 24, transcendentals=0),
        )(points, mean_vecs.reshape(4, 4, 4, 2, 2, 8, 512), log_w.reshape(16, 128), inv_temp)
        return out_mu.reshape(2048, 512), out_lw.reshape(2048), out_lse.reshape(n_pts)

    row_spec = P(("fit", "pts"))
    comp_spec = P(("fit", "comp"))
    return jax.shard_map(
        per_device,
        mesh=mesh,
        in_specs=(P(("fit", "pts"), None), P(("fit", "comp"), None), comp_spec, P()),
        out_specs=(P(("fit", "comp"), None), comp_spec, row_spec),
        check_vma=False,
    )
```

```python
import functools
import math

import jax
import jax.numpy as jnp
from jax import lax
from jax.experimental import pallas as pl
from jax.experimental.pallas import tpu as pltpu
from jax.sharding import PartitionSpec as P

PRIOR_ALPHA = 1e-3
COUNT_EPS = 1e-6
LOG2E = math.log2(math.e)
LN2 = math.log(2.0)
F32, BF16 = jnp.float32, jnp.bfloat16
MESH = pl.DeviceIdType.MESH

DIMS = ("z", "y", "x")
ORDERS = (("x", "y", "z"), ("y", "z", "x"), ("z", "x", "y"))
SUM_TILES = ((0, 3), (3, 6), (6, 9))
BF_TILES = (((0, 2), (2, 3), (3, 4)), ((0, 1), (1, 2), (2, 4)))
PB = 512
KC = 512


def cat(parts, axis):
    return jnp.concatenate(parts, axis=axis)


def kernel(n_total, k_total, sweeps, x_hbm, mean_hbm, lw_ref, beta_ref, out_mu, out_lw, out_lse,
           xv, e_ref, l0, l1, s_ref, muf, mu, ct, hrep, lrep, st, stp, wrow, qh,
           ra0, ra1, ra2, rb0, rb1, rb2, rc0, rc1, rc2,
           load_sem, ex_send, ex_recv, rs_send, rs_recv, ag_send, ag_recv):
    n_pts = xv.shape[0]
    nb = n_pts // PB
    fit, comp, pts = lax.axis_index("fit"), lax.axis_index("comp"), lax.axis_index("pts")
    me = {"z": lax.div(pts, 16), "y": lax.rem(lax.div(pts, 4), 4), "x": lax.rem(pts, 4)}
    near = {r: {d: lax.rem(me[d] + r, 4) for d in DIMS} for r in (1, 2, 3)}
    bufs = ((ra0, ra1, ra2), (rb0, rb1, rb2), (rc0, rc1, rc2))
    own = (me["z"], me["y"], me["x"])
    lane = lax.broadcasted_iota(jnp.int32, (8, 128), 1)

    def dev(d, r):
        c = {**me, d: near[r][d]}
        return (fit, comp, c["z"] * 16 + c["y"] * 4 + c["x"])

    def coord(d, r):
        return near[r][d] if r else me[d]

    def place(p, k, r, half=None):
        order = ORDERS[p]
        sel = {order[j]: me[order[j]] for j in range(k)}
        sel[order[k]] = coord(order[k], r)
        if half is not None:
            sel[order[2]] = pl.ds(2 * half, 2)
        return tuple(sel.get(d, slice(None)) for d in DIMS)

    def remote(src, dst, ss, rs, device):
        return pltpu.make_async_remote_copy(src_ref=src, dst_ref=dst, send_sem=ss, recv_sem=rs,
                                            device_id=device, device_id_type=MESH)

    def sums(h, p):
        return (h, pl.ds(SUM_TILES[p][0], SUM_TILES[p][1] - SUM_TILES[p][0]))

    def rs_copy(h, p, k, i):
        d, buf = ORDERS[p][k], bufs[k][p]
        if k == 2:
            r = (1, 3, 2)[i]
            src = s_ref.at[sums(h, p) + place(p, k, r)]
        else:
            r = (1, 3, 1, 1, 3, 3)[i]
            if i in (2, 5):
                src = buf.at[h, 0 if i == 2 else 1]
            else:
                to, half = {0: (2, 0), 1: (2, 1), 3: (1, 1), 4: (3, 0)}[i]
                src = s_ref.at[sums(h, p) + place(p, k, to, half)]
        j = 6 * k + i
        return remote(src, buf.at[h, i], rs_send.at[h, p, j], rs_recv.at[h, p, j], dev(d, r))

    def rs_start(h, k):
        for i in ((2, 0, 1) if k == 2 else (0, 1, 3, 4)):
            for p in range(3):
                rs_copy(h, p, k, i).start()

    def rs_relay(h, k):
        for p in range(3):
            buf = bufs[k][p]
            for i, to, half, nxt in ((0, 1, 0, 2), (1, 3, 1, 5)):
                rs_copy(h, p, k, i).wait_recv()
                buf[h, i] = buf[h, i] + s_ref[sums(h, p) + place(p, k, to, half)]
                rs_copy(h, p, k, nxt).start()

    def rs_finish(h, k):
        for p in range(3):
            buf = bufs[k][p]
            if k == 2:
                for i in range(3):
                    rs_copy(h, p, k, i).wait()
                mine = sums(h, p) + own
                s_ref[mine] = (s_ref[mine] + buf[h, 0]) + (buf[h, 1] + buf[h, 2])
                continue
            for half, i, j in ((0, 2, 4), (1, 3, 5)):
                rs_copy(h, p, k, i).wait_recv()
                rs_copy(h, p, k, j).wait_recv()
                mine = sums(h, p) + place(p, k, 0, half)
                s_ref[mine] = s_ref[mine] + (buf[h, i] + buf[h, j])
            for i in range(6):
                rs_copy(h, p, k, i).wait_send()

    def bf_units(h):
        units = []
        for p, (lo, hi) in enumerate(BF_TILES[h]):
            units.append((mu, (h, pl.ds(lo, hi - lo)), p))
        return units + [(ct, (h,), 1)]

    def f32_units(h):
        return [(muf, sums(h, p), p) for p in range(3)]

    def ag_copy(units, h, u, k, i):
        ref, lead, p = units[u]
        d = ORDERS[p][k]
        if k == 2:
            r = (1, 3, 2)[i]
            view = ref.at[lead + place(p, k, 0)]
        else:
            frm, half, r = ((0, 0, 1), (0, 1, 3), (0, 1, 1), (0, 0, 3), (3, 0, 1), (1, 1, 3))[i]
            view = ref.at[lead + place(p, k, frm, half)]
        j = 6 * k + i
        return remote(view, view, ag_send.at[h, u, j], ag_recv.at[h, u, j], dev(d, r))

    def ag_start(units, h, k):
        for i in ((2, 0, 1) if k == 2 else range(4)):
            for u in range(len(units)):
                ag_copy(units, h, u, k, i).start()

    def ag_relay(units, h, k):
        for u in range(len(units)):
            for i, nxt in ((0, 4), (1, 5)):
                ag_copy(units, h, u, k, i).wait_recv()
                ag_copy(units, h, u, k, nxt).start()

    def ag_finish(units, h, k):
        for u in range(len(units)):
            if k == 2:
                for i in range(3):
                    ag_copy(units, h, u, k, i).wait()
                continue
            for i in range(2, 6):
                ag_copy(units, h, u, k, i).wait_recv()
            for i in range(6):
                ag_copy(units, h, u, k, i).wait_send()

    def column(v, lanes):
        return jnp.broadcast_to(v[:, lanes:lanes + 1], (v.shape[0], 128))

    def expand(h):
        t = ct[h].reshape(512, 128)
        for hh in range(2):
            hrep[h, hh] = column(t, 32 * hh)
            lrep[h, hh] = column(t, 64 + 32 * hh) * LOG2E

    def logits(h, j, lref, b2):
        cols = pl.ds(pl.multiple_of(j * PB, PB), PB)
        xj = xv[cols, :]
        q = qh[:, cols]
        rows = cat([mu[h, c].reshape(1024, 128) for c in range(4)], 1)
        a = lax.dot_general(rows, xj, (((1,), (1,)), ((), ())), preferred_element_type=F32)
        a = a.reshape(64, 2, 8, PB)
        top = None
        for hh in range(2):
            hc = cat([hrep[h, hh]] * (PB // 128), 1)
            lc = cat([lrep[h, hh]] * (PB // 128), 1)
            v = ((a[:, hh].reshape(512, PB) - hc) - q) * b2 + lc
            lref[hh] = v
            t = jnp.max(v.reshape(64, 8, PB), axis=0)
            top = t if top is None else jnp.maximum(top, t)
        st[2 * h, :, cols] = jnp.max(top, axis=0, keepdims=True)

    def exps(h, j, lref):
        cols = pl.ds(pl.multiple_of(j * PB, PB), PB)
        m = st[2 * h, :, cols]
        tot = None
        for hh in range(2):
            e = jnp.exp2(lref[hh] - m)
            e_ref[2 * h + hh, :, cols] = e
            t = jnp.sum(e.reshape(64, 8, PB), axis=0)
            tot = t if tot is None else tot + t
        st[2 * h + 1, :, cols] = jnp.sum(tot, axis=0, keepdims=True)

    def scores(h, b2, during=()):
        logits(h, 0, l0, b2)

        @pl.loop(0, nb // 2 - 1)
        def _(i):
            for n, step in enumerate(during):
                pl.when(i == n)(step)
            logits(h, 2 * i + 1, l1, b2)
            exps(h, 2 * i, l0)
            logits(h, 2 * i + 2, l0, b2)
            exps(h, 2 * i + 1, l1)

        logits(h, nb - 1, l1, b2)
        exps(h, nb - 2, l0)
        exps(h, nb - 1, l1)

    def normalise(slot):
        ex = remote(st, stp.at[slot], ex_send, ex_recv.at[slot], (fit, 1 - comp, pts))
        ex.start()
        for h in range(2):
            s_ref[h, 8] = jnp.zeros((4, 4, 4, 8, 128), F32)
        ex.wait()
        tops = [st[0], st[2], stp[slot, 0], stp[slot, 2]]
        mm = jnp.maximum(jnp.maximum(tops[0], tops[1]), jnp.maximum(tops[2], tops[3]))
        tot = (st[1] * jnp.exp2(tops[0] - mm) + st[3] * jnp.exp2(tops[1] - mm)) + (
            stp[slot, 1] * jnp.exp2(tops[2] - mm) + stp[slot, 3] * jnp.exp2(tops[3] - mm))
        lse2 = mm + jnp.log2(tot)
        for h in range(2):
            wrow[h] = jnp.exp2(tops[h] - lse2)
        return lse2

    def moments():
        @pl.loop(0, 4)
        def _(r4):
            h, hh = lax.div(r4, 2), lax.rem(r4, 2)
            pl.when(r4 == 2)(lambda: rs_start(0, 0))
            pl.when(r4 == 3)(lambda: rs_relay(0, 0))
            acc, cnt = None, None
            for kc in range(n_pts // KC):
                k0 = kc * KC
                r = e_ref[r4, :, k0:k0 + KC] * wrow[h, :, k0:k0 + KC]
                for t in range(KC // 128):
                    rt = r[:, t * 128:(t + 1) * 128]
                    cnt = rt if cnt is None else cnt + rt
                part = jnp.dot(r.astype(BF16), xv[k0:k0 + KC, :], preferred_element_type=F32)
                acc = part if acc is None else acc + part
            for c in range(4):
                s_ref[h, hh * 4 + c] = acc[:, c * 128:(c + 1) * 128].reshape(4, 4, 4, 8, 128)
            cb = jnp.broadcast_to(jnp.sum(cnt, axis=1, keepdims=True), (512, 128)).reshape(64, 8, 128)
            cb = jnp.where(lax.div(lane, 64) == hh, cb, 0.0)
            s_ref[h, 8] = s_ref[h, 8] + cb.reshape(4, 4, 4, 8, 128)

    def update(h):
        ntile = s_ref[(h, 8) + own]
        vals, tile = [], jnp.zeros((8, 128), F32)
        for hh in range(2):
            n = column(ntile, 64 * hh)
            row = [s_ref[(h, hh * 4 + c) + own] / (n + COUNT_EPS) for c in range(4)]
            vals.append(row)
            sq = (row[0] * row[0] + row[1] * row[1]) + (row[2] * row[2] + row[3] * row[3])
            hc = jnp.broadcast_to(0.5 * jnp.sum(sq, axis=1, keepdims=True), (8, 128))
            lw = jnp.log((n + PRIOR_ALPHA) / (n_total + k_total * PRIOR_ALPHA))
            tile = jnp.where(lax.div(lane, 32) == hh, hc, tile)
            tile = jnp.where(lax.div(lane, 32) == 2 + hh, lw, tile)
        return vals, tile

    def update_bf(h):
        vals, tile = update(h)
        for c in range(4):
            mu[(h, c) + own] = cat([vals[0][c], vals[1][c]], 0).astype(BF16)
        ct[(h,) + own] = tile

    def update_f32(h):
        vals, tile = update(h)
        for hh in range(2):
            for c in range(4):
                muf[(h, hh * 4 + c) + own] = vals[hh][c]
        muf[(h, 8) + own] = tile

    def exchange(units, upd):
        rs_start(1, 0)
        rs_finish(0, 0)
        rs_relay(1, 0)
        rs_finish(1, 0)
        for k in (1, 2):
            for h in range(2):
                rs_start(h, k)
            if k == 1:
                for h in range(2):
                    rs_relay(h, k)
            for h in range(2):
                rs_finish(h, k)
        for h in range(2):
            upd(h)
        for k in (2, 1):
            for h in range(2):
                ag_start(units[h], h, k)
            if k == 1:
                for h in range(2):
                    ag_relay(units[h], h, k)
            for h in range(2):
                ag_finish(units[h], h, k)
        ag_start(units[0], 0, 0)
        ag_relay(units[0], 0, 0)
        ag_start(units[1], 1, 0)
        ag_finish(units[0], 0, 0)

    bar = pltpu.get_barrier_semaphore()
    pl.semaphore_signal(bar, inc=1, device_id=(fit, 1 - comp, pts), device_id_type=MESH)
    for d in DIMS:
        for r in (1, 2, 3):
            pl.semaphore_signal(bar, inc=1, device_id=dev(d, r), device_id_type=MESH)

    loads = [pltpu.make_async_copy(x_hbm, xv, load_sem.at[16])]
    for h in range(2):
        for hh in range(2):
            for c in range(4):
                t = hh * 4 + c
                loads.append(pltpu.make_async_copy(
                    mean_hbm.at[:, :, :, h, hh, :, pl.ds(c * 128, 128)], s_ref.at[h, t], load_sem.at[8 * h + t]))
    for c in loads[1:] + loads[:1]:
        c.start()
    for c in loads[1:]:
        c.wait()
    st[...] = jnp.zeros_like(st)

    @pl.loop(0, 2)
    def _(h):
        for hh in range(2):
            v = [s_ref[h, hh * 4 + c].reshape(512, 128) for c in range(4)]
            sq = (v[0] * v[0] + v[1] * v[1]) + (v[2] * v[2] + v[3] * v[3])
            hrep[h, hh] = jnp.broadcast_to(0.5 * jnp.sum(sq, axis=1, keepdims=True), (512, 128))
        for c in range(4):
            v = cat([s_ref[h, c].reshape(64, 8, 128), s_ref[h, 4 + c].reshape(64, 8, 128)], 1)
            mu[h, c] = v.astype(BF16).reshape(4, 4, 4, 16, 128)

    for i in range(16):
        col = jnp.broadcast_to(lw_ref[i:i + 1, :] * LOG2E, (128, 128)).T
        for g in range(4):
            for r4 in range(4):
                lo = 32 * g + 8 * r4
                lrep[r4 // 2, r4 % 2, (4 * i + g) * 8:(4 * i + g) * 8 + 8, :] = col[lo:lo + 8, :]
    loads[0].wait()

    @pl.loop(0, n_pts // 128)
    def _(i):
        rows = pl.ds(pl.multiple_of(i * 128, 128), 128)
        xb = xv[rows, :].astype(F32)
        sq = xb * xb
        sq = (sq[:, 0:128] + sq[:, 128:256]) + (sq[:, 256:384] + sq[:, 384:512])
        qh[:, rows] = jnp.sum(sq.T, axis=0, keepdims=True) * 0.5

    @pl.loop(0, 2)
    def _(h):
        scores(h, beta_ref[0] * (2.0 * LOG2E))

    pl.semaphore_wait(bar, 10)

    bf = (bf_units(0), bf_units(1))

    @pl.loop(0, sweeps - 1)
    def _(sweep):
        b2 = beta_ref[sweep + 1] * (2.0 * LOG2E)
        normalise(lax.rem(sweep, 2))
        moments()
        exchange(bf, update_bf)
        expand(0)

        scores(0, b2, (lambda: ag_relay(bf[1], 1, 0),))
        ag_finish(bf[1], 1, 0)
        expand(1)
        scores(1, b2)

    out_lse[...] = normalise((sweeps - 1) % 2) * LN2
    moments()
    f32 = (f32_units(0), f32_units(1))
    exchange(f32, update_f32)
    stores = []
    for h in range(2):
        if h == 1:
            ag_relay(f32[1], 1, 0)
        for hh in range(2):
            for c in range(4):
                t = hh * 4 + c
                stores.append(pltpu.make_async_copy(
                    muf.at[h, t], out_mu.at[:, :, :, h, hh, :, pl.ds(c * 128, 128)], load_sem.at[8 * h + t]))
                if h == 0:
                    stores[-1].start()
    ag_finish(f32[1], 1, 0)
    for c in stores[8:]:
        c.start()
    for i in range(16):
        tiles = []
        for g in range(4):
            for r4 in range(4):
                tiles.append(column(muf[r4 // 2, 8, i // 4, i % 4, g], 64 + 32 * (r4 % 2)))
        out_lw[i:i + 1, :] = cat(tiles, 0).T[0:1, :]
    for c in stores:
        c.wait()


def solution(mesh):
    row_groups = mesh.shape["pts"]
    comp_groups = mesh.shape["comp"]

    def per_device(points, mean_vecs, log_w, inv_temp):
        n_pts = points.shape[0]
        n_total = n_pts * row_groups
        k_total = mean_vecs.shape[0] * comp_groups
        sweeps = inv_temp.shape[0]

        def rbuf(k):
            shapes = []
            for (lo, hi), order in zip(SUM_TILES, ORDERS):
                if k == 2:
                    shapes.append(pltpu.VMEM((2, 3, hi - lo, 8, 128), F32))
                    continue
                dims = [2 if d == order[2] else 4 for d in DIMS if d not in order[:k + 1]]
                shapes.append(pltpu.VMEM((2, 6, hi - lo, *dims, 8, 128), F32))
            return shapes

        any_spec = pl.BlockSpec(memory_space=pl.ANY)
        vmem_spec = pl.BlockSpec(memory_space=pltpu.VMEM)
        out_mu, out_lw, out_lse = pl.pallas_call(
            functools.partial(kernel, n_total, k_total, sweeps),
            out_shape=(jax.ShapeDtypeStruct((4, 4, 4, 2, 2, 8, 512), F32),
                       jax.ShapeDtypeStruct((16, 128), F32),
                       jax.ShapeDtypeStruct((1, n_pts), F32)),
            in_specs=[any_spec, any_spec, vmem_spec, pl.BlockSpec(memory_space=pltpu.SMEM)],
            out_specs=(any_spec, vmem_spec, vmem_spec),
            scratch_shapes=[
                pltpu.VMEM((n_pts, 512), BF16),
                pltpu.VMEM((4, 512, n_pts), F32),
                pltpu.VMEM((2, 512, PB), F32),
                pltpu.VMEM((2, 512, PB), F32),
                pltpu.VMEM((2, 9, 4, 4, 4, 8, 128), F32),
                pltpu.VMEM((2, 9, 4, 4, 4, 8, 128), F32),
                pltpu.VMEM((2, 4, 4, 4, 4, 16, 128), BF16),
                pltpu.VMEM((2, 4, 4, 4, 8, 128), F32),
                pltpu.VMEM((2, 2, 512, 128), F32),
                pltpu.VMEM((2, 2, 512, 128), F32),
                pltpu.VMEM((4, 1, n_pts), F32),
                pltpu.VMEM((2, 4, 1, n_pts), F32),
                pltpu.VMEM((2, 1, n_pts), F32),
                pltpu.VMEM((1, n_pts), F32),
                *rbuf(0), *rbuf(1), *rbuf(2),
                pltpu.SemaphoreType.DMA((17,)),
                pltpu.SemaphoreType.DMA,
                pltpu.SemaphoreType.DMA((2,)),
                pltpu.SemaphoreType.DMA((2, 3, 15)),
                pltpu.SemaphoreType.DMA((2, 3, 15)),
                pltpu.SemaphoreType.DMA((2, 4, 15)),
                pltpu.SemaphoreType.DMA((2, 4, 15)),
            ],
            compiler_params=pltpu.CompilerParams(has_side_effects=True, collective_id=0, vmem_limit_bytes=67043328),
            cost_estimate=pl.CostEstimate(flops=6 * 2 * n_pts * 2048 * 512, bytes_accessed=1 << 24, transcendentals=0),
        )(points, mean_vecs.reshape(4, 4, 4, 2, 2, 8, 512), log_w.reshape(16, 128), inv_temp)
        return out_mu.reshape(2048, 512), out_lw.reshape(2048), out_lse.reshape(n_pts)

    row_spec = P(("fit", "pts"))
    comp_spec = P(("fit", "comp"))
    return jax.shard_map(
        per_device,
        mesh=mesh,
        in_specs=(P(("fit", "pts"), None), P(("fit", "comp"), None), comp_spec, P()),
        out_specs=(P(("fit", "comp"), None), comp_spec, row_spec),
        check_vma=False,
    )
```

```python
import functools
import math

import jax
import jax.numpy as jnp
from jax import lax
from jax.experimental import pallas as pl
from jax.experimental.pallas import tpu as pltpu
from jax.sharding import PartitionSpec as P

PRIOR_ALPHA = 1e-3
COUNT_EPS = 1e-6
LOG2E = math.log2(math.e)
LN2 = math.log(2.0)
F32, BF16 = jnp.float32, jnp.bfloat16
MESH = pl.DeviceIdType.MESH

DIMS = ("z", "y", "x")
ORDERS = (("x", "y", "z"), ("y", "z", "x"), ("z", "x", "y"))
SUM_TILES = ((0, 3), (3, 6), (6, 9))
BF_TILES = (((0, 2), (2, 3), (3, 4)), ((0, 1), (1, 2), (2, 4)))
PB = 512
KC = 512


def cat(parts, axis):
    return jnp.concatenate(parts, axis=axis)


def kernel(n_total, k_total, sweeps, x_hbm, mean_hbm, lw_ref, beta_ref, muf, out_lse,
           xv, e_ref, l0, l1, s_ref, mu, ct, hrep, lrep, st, stp, wrow, qh,
           ra0, ra1, ra2, rb0, rb1, rb2, rc0, rc1, rc2,
           load_sem, ex_send, ex_recv, rs_send, rs_recv, ag_send, ag_recv):
    n_pts = xv.shape[0]
    nb = n_pts // PB
    fit, comp, pts = lax.axis_index("fit"), lax.axis_index("comp"), lax.axis_index("pts")
    me = {"z": lax.div(pts, 16), "y": lax.rem(lax.div(pts, 4), 4), "x": lax.rem(pts, 4)}
    near = {r: {d: lax.rem(me[d] + r, 4) for d in DIMS} for r in (1, 2, 3)}
    bufs = ((ra0, ra1, ra2), (rb0, rb1, rb2), (rc0, rc1, rc2))
    own = (me["z"], me["y"], me["x"])
    lane = lax.broadcasted_iota(jnp.int32, (8, 128), 1)

    def dev(d, r):
        c = {**me, d: near[r][d]}
        return (fit, comp, c["z"] * 16 + c["y"] * 4 + c["x"])

    def coord(d, r):
        return near[r][d] if r else me[d]

    def place(p, k, r, half=None):
        order = ORDERS[p]
        sel = {order[j]: me[order[j]] for j in range(k)}
        sel[order[k]] = coord(order[k], r)
        if half is not None:
            sel[order[2]] = pl.ds(2 * half, 2)
        return tuple(sel.get(d, slice(None)) for d in DIMS)

    def remote(src, dst, ss, rs, device):
        return pltpu.make_async_remote_copy(src_ref=src, dst_ref=dst, send_sem=ss, recv_sem=rs,
                                            device_id=device, device_id_type=MESH)

    def sums(h, p):
        return (h, pl.ds(SUM_TILES[p][0], SUM_TILES[p][1] - SUM_TILES[p][0]))

    def rs_copy(h, p, k, i):
        d, buf = ORDERS[p][k], bufs[k][p]
        if k == 2:
            r = (1, 3, 2)[i]
            src = s_ref.at[sums(h, p) + place(p, k, r)]
        else:
            r = (1, 3, 1, 1, 3, 3)[i]
            if i in (2, 5):
                src = buf.at[h, 0 if i == 2 else 1]
            else:
                to, half = {0: (2, 0), 1: (2, 1), 3: (1, 1), 4: (3, 0)}[i]
                src = s_ref.at[sums(h, p) + place(p, k, to, half)]
        j = 6 * k + i
        return remote(src, buf.at[h, i], rs_send.at[h, p, j], rs_recv.at[h, p, j], dev(d, r))

    def rs_start(h, k, which=(0, 1, 3, 4)):
        for i in ((2, 0, 1) if k == 2 else which):
            for p in range(3):
                rs_copy(h, p, k, i).start()

    def rs_relay(h, k):
        for p in range(3):
            buf = bufs[k][p]
            for i, to, half, nxt in ((0, 1, 0, 2), (1, 3, 1, 5)):
                rs_copy(h, p, k, i).wait_recv()
                buf[h, i] = buf[h, i] + s_ref[sums(h, p) + place(p, k, to, half)]
                rs_copy(h, p, k, nxt).start()

    def rs_finish(h, k):
        for p in range(3):
            buf = bufs[k][p]
            if k == 2:
                for i in range(3):
                    rs_copy(h, p, k, i).wait()
                mine = sums(h, p) + own
                s_ref[mine] = (s_ref[mine] + buf[h, 0]) + (buf[h, 1] + buf[h, 2])
                continue
            for half, i, j in ((0, 2, 4), (1, 3, 5)):
                rs_copy(h, p, k, i).wait_recv()
                rs_copy(h, p, k, j).wait_recv()
                mine = sums(h, p) + place(p, k, 0, half)
                s_ref[mine] = s_ref[mine] + (buf[h, i] + buf[h, j])
            for i in range(6):
                rs_copy(h, p, k, i).wait_send()

    def bf_units(h):
        units = []
        for p, (lo, hi) in enumerate(BF_TILES[h]):
            units.append((mu, (h, pl.ds(lo, hi - lo)), p))
        return units + [(ct, (h,), 1)]

    def f32_units(h):
        return [(muf, sums(h, p), p) for p in range(3)]

    def ag_copy(units, h, u, k, i):
        ref, lead, p = units[u]
        d = ORDERS[p][k]
        if k == 2:
            r = (1, 3, 2)[i]
            view = ref.at[lead + place(p, k, 0)]
        else:
            frm, half, r = ((0, 0, 1), (0, 1, 3), (0, 1, 1), (0, 0, 3), (3, 0, 1), (1, 1, 3))[i]
            view = ref.at[lead + place(p, k, frm, half)]
        j = 6 * k + i
        return remote(view, view, ag_send.at[h, u, j], ag_recv.at[h, u, j], dev(d, r))

    def ag_start(units, h, k):
        for i in ((2, 0, 1) if k == 2 else range(4)):
            for u in range(len(units)):
                ag_copy(units, h, u, k, i).start()

    def ag_relay(units, h, k):
        for u in range(len(units)):
            for i, nxt in ((0, 4), (1, 5)):
                ag_copy(units, h, u, k, i).wait_recv()
                ag_copy(units, h, u, k, nxt).start()

    def ag_finish(units, h, k):
        for u in range(len(units)):
            if k == 2:
                for i in range(3):
                    ag_copy(units, h, u, k, i).wait()
                continue
            for i in range(2, 6):
                ag_copy(units, h, u, k, i).wait_recv()
            for i in range(6):
                ag_copy(units, h, u, k, i).wait_send()

    def column(v, lanes):
        return jnp.broadcast_to(v[:, lanes:lanes + 1], (v.shape[0], 128))

    def expand(h):
        t = ct[h].reshape(512, 128)
        for hh in range(2):
            hrep[h, hh] = column(t, 32 * hh)
            lrep[h, hh] = column(t, 64 + 32 * hh) * LOG2E

    def logits(h, j, lref, b2):
        cols = pl.ds(pl.multiple_of(j * PB, PB), PB)
        xj = xv[cols, :]
        q = qh[:, cols]
        rows = cat([mu[h, c].reshape(1024, 128) for c in range(4)], 1)
        a = lax.dot_general(rows, xj, (((1,), (1,)), ((), ())), preferred_element_type=F32)
        a = a.reshape(64, 2, 8, PB)
        top = None
        for hh in range(2):
            hc = cat([hrep[h, hh]] * (PB // 128), 1)
            lc = cat([lrep[h, hh]] * (PB // 128), 1)
            v = ((a[:, hh].reshape(512, PB) - hc) - q) * b2 + lc
            lref[hh] = v
            t = jnp.max(v.reshape(64, 8, PB), axis=0)
            top = t if top is None else jnp.maximum(top, t)
        st[2 * h, :, cols] = jnp.max(top, axis=0, keepdims=True)

    def exps(h, j, lref):
        cols = pl.ds(pl.multiple_of(j * PB, PB), PB)
        m = st[2 * h, :, cols]
        tot = None
        for hh in range(2):
            e = jnp.exp2(lref[hh] - m)
            e_ref[2 * h + hh, :, cols] = e
            t = jnp.sum(e.reshape(64, 8, PB), axis=0)
            tot = t if tot is None else tot + t
        st[2 * h + 1, :, cols] = jnp.sum(tot, axis=0, keepdims=True)

    def scores(h, b2, during=()):
        logits(h, 0, l0, b2)

        @pl.loop(0, nb // 2 - 1)
        def _(i):
            for n, step in enumerate(during):
                pl.when(i == n)(step)
            logits(h, 2 * i + 1, l1, b2)
            exps(h, 2 * i, l0)
            logits(h, 2 * i + 2, l0, b2)
            exps(h, 2 * i + 1, l1)

        logits(h, nb - 1, l1, b2)
        exps(h, nb - 2, l0)
        exps(h, nb - 1, l1)

    def normalise(slot):
        ex = remote(st, stp.at[slot], ex_send, ex_recv.at[slot], (fit, 1 - comp, pts))
        ex.start()
        for h in range(2):
            s_ref[h, 8] = jnp.zeros((4, 4, 4, 8, 128), F32)
        ex.wait()
        tops = [st[0], st[2], stp[slot, 0], stp[slot, 2]]
        mm = jnp.maximum(jnp.maximum(tops[0], tops[1]), jnp.maximum(tops[2], tops[3]))
        tot = (st[1] * jnp.exp2(tops[0] - mm) + st[3] * jnp.exp2(tops[1] - mm)) + (
            stp[slot, 1] * jnp.exp2(tops[2] - mm) + stp[slot, 3] * jnp.exp2(tops[3] - mm))
        lse2 = mm + jnp.log2(tot)
        for h in range(2):
            wrow[h] = jnp.exp2(tops[h] - lse2)
        return lse2

    def moments():
        @pl.loop(0, 4)
        def _(r4):
            h, hh = lax.div(r4, 2), lax.rem(r4, 2)
            pl.when(r4 == 2)(lambda: rs_start(0, 0))
            pl.when(r4 == 3)(lambda: rs_relay(0, 0))
            acc, cnt = None, None
            for kc in range(n_pts // KC):
                k0 = kc * KC
                r = e_ref[r4, :, k0:k0 + KC] * wrow[h, :, k0:k0 + KC]
                for t in range(KC // 128):
                    rt = r[:, t * 128:(t + 1) * 128]
                    cnt = rt if cnt is None else cnt + rt
                part = jnp.dot(r.astype(BF16), xv[k0:k0 + KC, :], preferred_element_type=F32)
                acc = part if acc is None else acc + part
            for c in range(4):
                s_ref[h, hh * 4 + c] = acc[:, c * 128:(c + 1) * 128].reshape(4, 4, 4, 8, 128)
            cb = jnp.broadcast_to(jnp.sum(cnt, axis=1, keepdims=True), (512, 128)).reshape(64, 8, 128)
            cb = jnp.where(lax.div(lane, 64) == hh, cb, 0.0)
            s_ref[h, 8] = s_ref[h, 8] + cb.reshape(4, 4, 4, 8, 128)

    def update(h):
        ntile = s_ref[(h, 8) + own]
        vals, tile = [], jnp.zeros((8, 128), F32)
        for hh in range(2):
            n = column(ntile, 64 * hh)
            row = [s_ref[(h, hh * 4 + c) + own] / (n + COUNT_EPS) for c in range(4)]
            vals.append(row)
            sq = (row[0] * row[0] + row[1] * row[1]) + (row[2] * row[2] + row[3] * row[3])
            hc = jnp.broadcast_to(0.5 * jnp.sum(sq, axis=1, keepdims=True), (8, 128))
            lw = jnp.log((n + PRIOR_ALPHA) / (n_total + k_total * PRIOR_ALPHA))
            tile = jnp.where(lax.div(lane, 32) == hh, hc, tile)
            tile = jnp.where(lax.div(lane, 32) == 2 + hh, lw, tile)
        return vals, tile

    def update_bf(h):
        vals, tile = update(h)
        for c in range(4):
            mu[(h, c) + own] = cat([vals[0][c], vals[1][c]], 0).astype(BF16)
        ct[(h,) + own] = tile

    def update_f32(h):
        vals, tile = update(h)
        for hh in range(2):
            for c in range(4):
                muf[(h, hh * 4 + c) + own] = vals[hh][c]
        muf[(h, 8) + own] = tile

    def exchange(units, upd):
        u0, u1 = units
        rs_start(1, 0, (0, 1))
        rs_finish(0, 0)
        rs_start(0, 1)
        rs_start(1, 0, (3, 4))
        rs_relay(0, 1)
        rs_relay(1, 0)
        rs_finish(0, 1)
        rs_start(0, 2)
        rs_finish(1, 0)
        rs_start(1, 1)
        rs_finish(0, 2)
        upd(0)
        ag_start(u0, 0, 2)
        rs_relay(1, 1)
        ag_finish(u0, 0, 2)
        ag_start(u0, 0, 1)
        rs_finish(1, 1)
        rs_start(1, 2)
        ag_relay(u0, 0, 1)
        ag_finish(u0, 0, 1)
        ag_start(u0, 0, 0)
        rs_finish(1, 2)
        upd(1)
        ag_start(u1, 1, 2)
        ag_relay(u0, 0, 0)
        ag_finish(u1, 1, 2)
        ag_start(u1, 1, 1)
        ag_finish(u0, 0, 0)

    bar = pltpu.get_barrier_semaphore()
    pl.semaphore_signal(bar, inc=1, device_id=(fit, 1 - comp, pts), device_id_type=MESH)
    for d in DIMS:
        for r in (1, 2, 3):
            pl.semaphore_signal(bar, inc=1, device_id=dev(d, r), device_id_type=MESH)

    loads = [pltpu.make_async_copy(x_hbm, xv, load_sem.at[16])]
    for h in range(2):
        for hh in range(2):
            for c in range(4):
                t = hh * 4 + c
                loads.append(pltpu.make_async_copy(
                    mean_hbm.at[:, :, :, h, hh, :, pl.ds(c * 128, 128)], s_ref.at[h, t], load_sem.at[8 * h + t]))
    for c in loads[1:] + loads[:1]:
        c.start()
    for c in loads[1:]:
        c.wait()
    st[...] = jnp.zeros_like(st)

    @pl.loop(0, 2)
    def _(h):
        for hh in range(2):
            v = [s_ref[h, hh * 4 + c].reshape(512, 128) for c in range(4)]
            sq = (v[0] * v[0] + v[1] * v[1]) + (v[2] * v[2] + v[3] * v[3])
            hrep[h, hh] = jnp.broadcast_to(0.5 * jnp.sum(sq, axis=1, keepdims=True), (512, 128))
        for c in range(4):
            v = cat([s_ref[h, c].reshape(64, 8, 128), s_ref[h, 4 + c].reshape(64, 8, 128)], 1)
            mu[h, c] = v.astype(BF16).reshape(4, 4, 4, 16, 128)

    for i in range(16):
        col = jnp.broadcast_to(lw_ref[i:i + 1, :] * LOG2E, (128, 128)).T
        for g in range(4):
            for r4 in range(4):
                lo = 32 * g + 8 * r4
                lrep[r4 // 2, r4 % 2, (4 * i + g) * 8:(4 * i + g) * 8 + 8, :] = col[lo:lo + 8, :]
    loads[0].wait()

    @pl.loop(0, n_pts // 128, unroll=4)
    def _(i):
        rows = pl.ds(pl.multiple_of(i * 128, 128), 128)
        xb = xv[rows, :].astype(F32)
        sq = xb * xb
        sq = (sq[:, 0:128] + sq[:, 128:256]) + (sq[:, 256:384] + sq[:, 384:512])
        qh[:, rows] = jnp.sum(sq.T, axis=0, keepdims=True) * 0.5

    @pl.loop(0, 2)
    def _(h):
        scores(h, beta_ref[0] * (2.0 * LOG2E))

    pl.semaphore_wait(bar, 10)

    bf = (bf_units(0), bf_units(1))

    @pl.loop(0, sweeps - 1)
    def _(sweep):
        b2 = beta_ref[sweep + 1] * (2.0 * LOG2E)
        normalise(lax.rem(sweep, 2))
        moments()
        exchange(bf, update_bf)
        expand(0)

        def next_phase():
            ag_finish(bf[1], 1, 1)
            ag_start(bf[1], 1, 0)

        scores(0, b2, (lambda: ag_relay(bf[1], 1, 1), next_phase, lambda: ag_relay(bf[1], 1, 0)))
        ag_finish(bf[1], 1, 0)
        expand(1)
        scores(1, b2)

    out_lse[...] = normalise((sweeps - 1) % 2) * LN2
    moments()
    f32 = (f32_units(0), f32_units(1))
    exchange(f32, update_f32)
    ag_relay(f32[1], 1, 1)
    ag_finish(f32[1], 1, 1)
    ag_start(f32[1], 1, 0)
    ag_relay(f32[1], 1, 0)
    ag_finish(f32[1], 1, 0)


def write_out(muf, lse, out_mu, out_lw, out_lse, sem):
    stores = []
    for h in range(2):
        for hh in range(2):
            for c in range(4):
                t = hh * 4 + c
                stores.append(pltpu.make_async_copy(
                    muf.at[h, t], out_mu.at[:, :, :, h, hh, :, pl.ds(c * 128, 128)], sem.at[8 * h + t]))
                stores[-1].start()
    for i in range(16):
        tiles = []
        for g in range(4):
            for r4 in range(4):
                v = muf[r4 // 2, 8, i // 4, i % 4, g]
                lo = 64 + 32 * (r4 % 2)
                tiles.append(jnp.broadcast_to(v[:, lo:lo + 1], (8, 128)))
        out_lw[i:i + 1, :] = cat(tiles, 0).T[0:1, :]
    out_lse[...] = lse[...]
    for c in stores:
        c.wait()


def solution(mesh):
    row_groups = mesh.shape["pts"]
    comp_groups = mesh.shape["comp"]

    def per_device(points, mean_vecs, log_w, inv_temp):
        n_pts = points.shape[0]
        n_total = n_pts * row_groups
        k_total = mean_vecs.shape[0] * comp_groups
        sweeps = inv_temp.shape[0]

        def rbuf(k):
            shapes = []
            for (lo, hi), order in zip(SUM_TILES, ORDERS):
                if k == 2:
                    shapes.append(pltpu.VMEM((2, 3, hi - lo, 8, 128), F32))
                    continue
                dims = [2 if d == order[2] else 4 for d in DIMS if d not in order[:k + 1]]
                shapes.append(pltpu.VMEM((2, 6, hi - lo, *dims, 8, 128), F32))
            return shapes

        any_spec = pl.BlockSpec(memory_space=pl.ANY)
        vmem_spec = pl.BlockSpec(memory_space=pltpu.VMEM)
        muf, lse = pl.pallas_call(
            functools.partial(kernel, n_total, k_total, sweeps),
            out_shape=(pltpu.VMEM((2, 9, 4, 4, 4, 8, 128), F32), pltpu.VMEM((1, n_pts), F32)),
            in_specs=[any_spec, any_spec, vmem_spec, pl.BlockSpec(memory_space=pltpu.SMEM)],
            out_specs=(vmem_spec, vmem_spec),
            scratch_shapes=[
                pltpu.VMEM((n_pts, 512), BF16),
                pltpu.VMEM((4, 512, n_pts), F32),
                pltpu.VMEM((2, 512, PB), F32),
                pltpu.VMEM((2, 512, PB), F32),
                pltpu.VMEM((2, 9, 4, 4, 4, 8, 128), F32),
                pltpu.VMEM((2, 4, 4, 4, 4, 16, 128), BF16),
                pltpu.VMEM((2, 4, 4, 4, 8, 128), F32),
                pltpu.VMEM((2, 2, 512, 128), F32),
                pltpu.VMEM((2, 2, 512, 128), F32),
                pltpu.VMEM((4, 1, n_pts), F32),
                pltpu.VMEM((2, 4, 1, n_pts), F32),
                pltpu.VMEM((2, 1, n_pts), F32),
                pltpu.VMEM((1, n_pts), F32),
                *rbuf(0), *rbuf(1), *rbuf(2),
                pltpu.SemaphoreType.DMA((17,)),
                pltpu.SemaphoreType.DMA,
                pltpu.SemaphoreType.DMA((2,)),
                pltpu.SemaphoreType.DMA((2, 3, 15)),
                pltpu.SemaphoreType.DMA((2, 3, 15)),
                pltpu.SemaphoreType.DMA((2, 4, 15)),
                pltpu.SemaphoreType.DMA((2, 4, 15)),
            ],
            compiler_params=pltpu.CompilerParams(has_side_effects=True, collective_id=0, vmem_limit_bytes=61000000),
            cost_estimate=pl.CostEstimate(flops=6 * 2 * n_pts * 2048 * 512, bytes_accessed=1 << 24, transcendentals=0),
        )(points, mean_vecs.reshape(4, 4, 4, 2, 2, 8, 512), log_w.reshape(16, 128), inv_temp)
        out_mu, out_lw, out_lse = pl.pallas_call(
            write_out,
            out_shape=(jax.ShapeDtypeStruct((4, 4, 4, 2, 2, 8, 512), F32),
                       jax.ShapeDtypeStruct((16, 128), F32),
                       jax.ShapeDtypeStruct((1, n_pts), F32)),
            in_specs=[vmem_spec, vmem_spec],
            out_specs=(any_spec, vmem_spec, vmem_spec),
            scratch_shapes=[pltpu.SemaphoreType.DMA((16,))],
            compiler_params=pltpu.CompilerParams(vmem_limit_bytes=16 << 20),
        )(muf, lse)
        return out_mu.reshape(2048, 512), out_lw.reshape(2048), out_lse.reshape(n_pts)

    row_spec = P(("fit", "pts"))
    comp_spec = P(("fit", "comp"))
    return jax.shard_map(
        per_device,
        mesh=mesh,
        in_specs=(P(("fit", "pts"), None), P(("fit", "comp"), None), comp_spec, P()),
        out_specs=(P(("fit", "comp"), None), comp_spec, row_spec),
        check_vma=False,
    )
```

```python
import functools
import math

import jax
import jax.numpy as jnp
from jax import lax
from jax.experimental import pallas as pl
from jax.experimental.pallas import tpu as pltpu
from jax.sharding import PartitionSpec as P

PRIOR_ALPHA = 1e-3
COUNT_EPS = 1e-6
LOG2E = math.log2(math.e)
LN2 = math.log(2.0)
F32, BF16 = jnp.float32, jnp.bfloat16
MESH = pl.DeviceIdType.MESH

DIMS = ("z", "y", "x")
ORDERS = (("x", "y", "z"), ("y", "z", "x"), ("z", "x", "y"))
SUM_TILES = ((0, 3), (3, 6), (6, 9))
BF_TILES = (((0, 2), (2, 3), (3, 4)), ((0, 1), (1, 2), (2, 4)))
PB = 512
KC = 512


def cat(parts, axis):
    return jnp.concatenate(parts, axis=axis)


def kernel(n_total, k_total, sweeps, x_hbm, mean_hbm, lw_ref, beta_ref, muf, out_lse,
           xv, e_ref, l0, l1, s_ref, mu, ct, hrep, lrep, st, stp, wrow, qh,
           ra0, ra1, ra2, rb0, rb1, rb2, rc0, rc1, rc2,
           load_sem, ex_send, ex_recv, rs_send, rs_recv, ag_send, ag_recv):
    n_pts = xv.shape[0]
    nb = n_pts // PB
    fit, comp, pts = lax.axis_index("fit"), lax.axis_index("comp"), lax.axis_index("pts")
    me = {"z": lax.div(pts, 16), "y": lax.rem(lax.div(pts, 4), 4), "x": lax.rem(pts, 4)}
    near = {r: {d: lax.rem(me[d] + r, 4) for d in DIMS} for r in (1, 2, 3)}
    bufs = ((ra0, ra1, ra2), (rb0, rb1, rb2), (rc0, rc1, rc2))
    own = (me["z"], me["y"], me["x"])
    lane = lax.broadcasted_iota(jnp.int32, (8, 128), 1)

    def dev(d, r):
        c = {**me, d: near[r][d]}
        return (fit, comp, c["z"] * 16 + c["y"] * 4 + c["x"])

    def coord(d, r):
        return near[r][d] if r else me[d]

    def place(p, k, r, half=None):
        order = ORDERS[p]
        sel = {order[j]: me[order[j]] for j in range(k)}
        sel[order[k]] = coord(order[k], r)
        if half is not None:
            sel[order[2]] = pl.ds(2 * half, 2)
        return tuple(sel.get(d, slice(None)) for d in DIMS)

    def remote(src, dst, ss, rs, device):
        return pltpu.make_async_remote_copy(src_ref=src, dst_ref=dst, send_sem=ss, recv_sem=rs,
                                            device_id=device, device_id_type=MESH)

    def sums(h, p):
        return (h, pl.ds(SUM_TILES[p][0], SUM_TILES[p][1] - SUM_TILES[p][0]))

    def rs_copy(h, p, k, i):
        d, buf = ORDERS[p][k], bufs[k][p]
        if k == 2:
            r = (1, 3, 2)[i]
            src = s_ref.at[sums(h, p) + place(p, k, r)]
        else:
            r = (1, 3, 1, 1, 3, 3)[i]
            if i in (2, 5):
                src = buf.at[h, 0 if i == 2 else 1]
            else:
                to, half = {0: (2, 0), 1: (2, 1), 3: (1, 1), 4: (3, 0)}[i]
                src = s_ref.at[sums(h, p) + place(p, k, to, half)]
        j = 6 * k + i
        return remote(src, buf.at[h, i], rs_send.at[h, p, j], rs_recv.at[h, p, j], dev(d, r))

    def rs_start(h, k, which=(0, 1, 3, 4)):
        for i in ((2, 0, 1) if k == 2 else which):
            for p in range(3):
                rs_copy(h, p, k, i).start()

    def rs_relay(h, k):
        for p in range(3):
            buf = bufs[k][p]
            for i, to, half, nxt in ((0, 1, 0, 2), (1, 3, 1, 5)):
                rs_copy(h, p, k, i).wait_recv()
                buf[h, i] = buf[h, i] + s_ref[sums(h, p) + place(p, k, to, half)]
                rs_copy(h, p, k, nxt).start()

    def rs_finish(h, k):
        for p in range(3):
            buf = bufs[k][p]
            if k == 2:
                for i in range(3):
                    rs_copy(h, p, k, i).wait()
                mine = sums(h, p) + own
                s_ref[mine] = (s_ref[mine] + buf[h, 0]) + (buf[h, 1] + buf[h, 2])
                continue
            for half, i, j in ((0, 2, 4), (1, 3, 5)):
                rs_copy(h, p, k, i).wait_recv()
                rs_copy(h, p, k, j).wait_recv()
                mine = sums(h, p) + place(p, k, 0, half)
                s_ref[mine] = s_ref[mine] + (buf[h, i] + buf[h, j])
            for i in range(6):
                rs_copy(h, p, k, i).wait_send()

    def bf_units(h):
        units = []
        for p, (lo, hi) in enumerate(BF_TILES[h]):
            units.append((mu, (h, pl.ds(lo, hi - lo)), p))
        return units + [(ct, (h,), 1)]

    def f32_units(h):
        return [(muf, sums(h, p), p) for p in range(3)]

    def ag_copy(units, h, u, k, i):
        ref, lead, p = units[u]
        d = ORDERS[p][k]
        if k == 2:
            r = (1, 3, 2)[i]
            view = ref.at[lead + place(p, k, 0)]
        else:
            frm, half, r = ((0, 0, 1), (0, 1, 3), (0, 1, 1), (0, 0, 3), (3, 0, 1), (1, 1, 3))[i]
            view = ref.at[lead + place(p, k, frm, half)]
        j = 6 * k + i
        return remote(view, view, ag_send.at[h, u, j], ag_recv.at[h, u, j], dev(d, r))

    def ag_start(units, h, k):
        for i in ((2, 0, 1) if k == 2 else range(4)):
            for u in range(len(units)):
                ag_copy(units, h, u, k, i).start()

    def ag_relay(units, h, k):
        for u in range(len(units)):
            for i, nxt in ((0, 4), (1, 5)):
                ag_copy(units, h, u, k, i).wait_recv()
                ag_copy(units, h, u, k, nxt).start()

    def ag_finish(units, h, k):
        for u in range(len(units)):
            if k == 2:
                for i in range(3):
                    ag_copy(units, h, u, k, i).wait()
                continue
            for i in range(2, 6):
                ag_copy(units, h, u, k, i).wait_recv()
            for i in range(6):
                ag_copy(units, h, u, k, i).wait_send()

    def column(v, lanes):
        return jnp.broadcast_to(v[:, lanes:lanes + 1], (v.shape[0], 128))

    def expand(h):
        t = ct[h].reshape(512, 128)
        for hh in range(2):
            hrep[h, hh] = column(t, 32 * hh)
            lrep[h, hh] = column(t, 64 + 32 * hh) * LOG2E

    def logits(h, j, lref, b2):
        cols = pl.ds(pl.multiple_of(j * PB, PB), PB)
        xj = xv[cols, :]
        q = qh[:, cols]
        rows = cat([mu[h, c].reshape(1024, 128) for c in range(4)], 1)
        a = lax.dot_general(rows, xj, (((1,), (1,)), ((), ())), preferred_element_type=F32)
        a = a.reshape(64, 2, 8, PB)
        top = None
        for hh in range(2):
            hc = cat([hrep[h, hh]] * (PB // 128), 1)
            lc = cat([lrep[h, hh]] * (PB // 128), 1)
            v = ((a[:, hh].reshape(512, PB) - hc) - q) * b2 + lc
            lref[hh] = v
            t = jnp.max(v.reshape(64, 8, PB), axis=0)
            top = t if top is None else jnp.maximum(top, t)
        st[2 * h, :, cols] = jnp.max(top, axis=0, keepdims=True)

    def exps(h, j, lref):
        cols = pl.ds(pl.multiple_of(j * PB, PB), PB)
        m = st[2 * h, :, cols]
        tot = None
        for hh in range(2):
            e = jnp.exp2(lref[hh] - m)
            e_ref[2 * h + hh, :, cols] = e
            t = jnp.sum(e.reshape(64, 8, PB), axis=0)
            tot = t if tot is None else tot + t
        st[2 * h + 1, :, cols] = jnp.sum(tot, axis=0, keepdims=True)

    def scores(h, b2, during=()):
        logits(h, 0, l0, b2)

        @pl.loop(0, nb // 2 - 1)
        def _(i):
            for n, step in enumerate(during):
                pl.when(i == n)(step)
            exps(h, 2 * i, l0)
            logits(h, 2 * i + 1, l1, b2)
            exps(h, 2 * i + 1, l1)
            logits(h, 2 * i + 2, l0, b2)

        logits(h, nb - 1, l1, b2)
        exps(h, nb - 2, l0)
        exps(h, nb - 1, l1)

    def normalise(slot):
        ex = remote(st, stp.at[slot], ex_send, ex_recv.at[slot], (fit, 1 - comp, pts))
        ex.start()
        for h in range(2):
            s_ref[h, 8] = jnp.zeros((4, 4, 4, 8, 128), F32)
        ex.wait()
        tops = [st[0], st[2], stp[slot, 0], stp[slot, 2]]
        mm = jnp.maximum(jnp.maximum(tops[0], tops[1]), jnp.maximum(tops[2], tops[3]))
        tot = (st[1] * jnp.exp2(tops[0] - mm) + st[3] * jnp.exp2(tops[1] - mm)) + (
            stp[slot, 1] * jnp.exp2(tops[2] - mm) + stp[slot, 3] * jnp.exp2(tops[3] - mm))
        lse2 = mm + jnp.log2(tot)
        for h in range(2):
            wrow[h] = jnp.exp2(tops[h] - lse2)
        return lse2

    def moments():
        @pl.loop(0, 4)
        def _(r4):
            h, hh = lax.div(r4, 2), lax.rem(r4, 2)
            pl.when(r4 == 2)(lambda: rs_start(0, 0))
            pl.when(r4 == 3)(lambda: rs_relay(0, 0))
            acc, cnt = None, None
            for kc in range(n_pts // KC):
                k0 = kc * KC
                r = e_ref[r4, :, k0:k0 + KC] * wrow[h, :, k0:k0 + KC]
                for t in range(KC // 128):
                    rt = r[:, t * 128:(t + 1) * 128]
                    cnt = rt if cnt is None else cnt + rt
                part = jnp.dot(r.astype(BF16), xv[k0:k0 + KC, :], preferred_element_type=F32)
                acc = part if acc is None else acc + part
            for c in range(4):
                s_ref[h, hh * 4 + c] = acc[:, c * 128:(c + 1) * 128].reshape(4, 4, 4, 8, 128)
            cb = jnp.broadcast_to(jnp.sum(cnt, axis=1, keepdims=True), (512, 128)).reshape(64, 8, 128)
            cb = jnp.where(lax.div(lane, 64) == hh, cb, 0.0)
            s_ref[h, 8] = s_ref[h, 8] + cb.reshape(4, 4, 4, 8, 128)

    def update(h):
        ntile = s_ref[(h, 8) + own]
        vals, tile = [], jnp.zeros((8, 128), F32)
        for hh in range(2):
            n = column(ntile, 64 * hh)
            row = [s_ref[(h, hh * 4 + c) + own] / (n + COUNT_EPS) for c in range(4)]
            vals.append(row)
            sq = (row[0] * row[0] + row[1] * row[1]) + (row[2] * row[2] + row[3] * row[3])
            hc = jnp.broadcast_to(0.5 * jnp.sum(sq, axis=1, keepdims=True), (8, 128))
            lw = jnp.log((n + PRIOR_ALPHA) / (n_total + k_total * PRIOR_ALPHA))
            tile = jnp.where(lax.div(lane, 32) == hh, hc, tile)
            tile = jnp.where(lax.div(lane, 32) == 2 + hh, lw, tile)
        return vals, tile

    def update_bf(h):
        vals, tile = update(h)
        for c in range(4):
            mu[(h, c) + own] = cat([vals[0][c], vals[1][c]], 0).astype(BF16)
        ct[(h,) + own] = tile

    def update_f32(h):
        vals, tile = update(h)
        for hh in range(2):
            for c in range(4):
                muf[(h, hh * 4 + c) + own] = vals[hh][c]
        muf[(h, 8) + own] = tile

    def exchange(units, upd):
        u0, u1 = units
        rs_start(1, 0, (0, 1))
        rs_finish(0, 0)
        rs_start(0, 1)
        rs_start(1, 0, (3, 4))
        rs_relay(0, 1)
        rs_relay(1, 0)
        rs_finish(0, 1)
        rs_start(0, 2)
        rs_finish(0, 2)
        upd(0)
        ag_start(u0, 0, 2)
        rs_finish(1, 0)
        rs_start(1, 1)
        ag_finish(u0, 0, 2)
        ag_start(u0, 0, 1)
        rs_relay(1, 1)
        ag_relay(u0, 0, 1)
        rs_finish(1, 1)
        rs_start(1, 2)
        ag_finish(u0, 0, 1)
        ag_start(u0, 0, 0)
        rs_finish(1, 2)
        upd(1)
        ag_start(u1, 1, 2)
        ag_relay(u0, 0, 0)
        ag_finish(u1, 1, 2)
        ag_start(u1, 1, 1)
        ag_finish(u0, 0, 0)

    bar = pltpu.get_barrier_semaphore()
    pl.semaphore_signal(bar, inc=1, device_id=(fit, 1 - comp, pts), device_id_type=MESH)
    for d in DIMS:
        for r in (1, 2, 3):
            pl.semaphore_signal(bar, inc=1, device_id=dev(d, r), device_id_type=MESH)

    loads = [pltpu.make_async_copy(x_hbm, xv, load_sem.at[16])]
    for h in range(2):
        for hh in range(2):
            for c in range(4):
                t = hh * 4 + c
                loads.append(pltpu.make_async_copy(
                    mean_hbm.at[:, :, :, h, hh, :, pl.ds(c * 128, 128)], s_ref.at[h, t], load_sem.at[8 * h + t]))
    for c in loads[1:9] + loads[:1] + loads[9:]:
        c.start()
    st[...] = jnp.zeros_like(st)
    for i in range(16):
        col = jnp.broadcast_to(lw_ref[i:i + 1, :] * LOG2E, (128, 128)).T
        for g in range(4):
            for r4 in range(4):
                lo = 32 * g + 8 * r4
                lrep[r4 // 2, r4 % 2, (4 * i + g) * 8:(4 * i + g) * 8 + 8, :] = col[lo:lo + 8, :]
    loads[0].wait()

    @pl.loop(0, n_pts // 128, unroll=4)
    def _(i):
        rows = pl.ds(pl.multiple_of(i * 128, 128), 128)
        xb = xv[rows, :].astype(F32)
        sq = xb * xb
        sq = (sq[:, 0:128] + sq[:, 128:256]) + (sq[:, 256:384] + sq[:, 384:512])
        qh[:, rows] = jnp.sum(sq.T, axis=0, keepdims=True) * 0.5

    for c in loads[1:]:
        c.wait()

    @pl.loop(0, 2)
    def _(h):
        for hh in range(2):
            v = [s_ref[h, hh * 4 + c].reshape(512, 128) for c in range(4)]
            sq = (v[0] * v[0] + v[1] * v[1]) + (v[2] * v[2] + v[3] * v[3])
            hrep[h, hh] = jnp.broadcast_to(0.5 * jnp.sum(sq, axis=1, keepdims=True), (512, 128))
        for c in range(4):
            v = cat([s_ref[h, c].reshape(64, 8, 128), s_ref[h, 4 + c].reshape(64, 8, 128)], 1)
            mu[h, c] = v.astype(BF16).reshape(4, 4, 4, 16, 128)
        scores(h, beta_ref[0] * (2.0 * LOG2E))

    pl.semaphore_wait(bar, 10)

    bf = (bf_units(0), bf_units(1))

    @pl.loop(0, sweeps - 1)
    def _(sweep):
        b2 = beta_ref[sweep + 1] * (2.0 * LOG2E)
        normalise(lax.rem(sweep, 2))
        moments()
        exchange(bf, update_bf)
        expand(0)

        def next_phase():
            ag_finish(bf[1], 1, 1)
            ag_start(bf[1], 1, 0)

        scores(0, b2, (lambda: ag_relay(bf[1], 1, 1), next_phase, lambda: ag_relay(bf[1], 1, 0)))
        ag_finish(bf[1], 1, 0)
        expand(1)
        scores(1, b2)

    out_lse[...] = normalise((sweeps - 1) % 2) * LN2
    moments()
    f32 = (f32_units(0), f32_units(1))
    exchange(f32, update_f32)
    ag_relay(f32[1], 1, 1)
    ag_finish(f32[1], 1, 1)
    ag_start(f32[1], 1, 0)
    ag_relay(f32[1], 1, 0)
    ag_finish(f32[1], 1, 0)


def write_out(muf, lse, out_mu, out_lw, out_lse, sem):
    stores = []
    for h in range(2):
        for hh in range(2):
            for c in range(4):
                t = hh * 4 + c
                stores.append(pltpu.make_async_copy(
                    muf.at[h, t], out_mu.at[:, :, :, h, hh, :, pl.ds(c * 128, 128)], sem.at[8 * h + t]))
                stores[-1].start()
    for i in range(16):
        tiles = []
        for g in range(4):
            for r4 in range(4):
                v = muf[r4 // 2, 8, i // 4, i % 4, g]
                lo = 64 + 32 * (r4 % 2)
                tiles.append(jnp.broadcast_to(v[:, lo:lo + 1], (8, 128)))
        out_lw[i:i + 1, :] = cat(tiles, 0).T[0:1, :]
    out_lse[...] = lse[...]
    for c in stores:
        c.wait()


def solution(mesh):
    row_groups = mesh.shape["pts"]
    comp_groups = mesh.shape["comp"]

    def per_device(points, mean_vecs, log_w, inv_temp):
        n_pts = points.shape[0]
        n_total = n_pts * row_groups
        k_total = mean_vecs.shape[0] * comp_groups
        sweeps = inv_temp.shape[0]

        def rbuf(k):
            shapes = []
            for (lo, hi), order in zip(SUM_TILES, ORDERS):
                if k == 2:
                    shapes.append(pltpu.VMEM((2, 3, hi - lo, 8, 128), F32))
                    continue
                dims = [2 if d == order[2] else 4 for d in DIMS if d not in order[:k + 1]]
                shapes.append(pltpu.VMEM((2, 6, hi - lo, *dims, 8, 128), F32))
            return shapes

        any_spec = pl.BlockSpec(memory_space=pl.ANY)
        vmem_spec = pl.BlockSpec(memory_space=pltpu.VMEM)
        muf, lse = pl.pallas_call(
            functools.partial(kernel, n_total, k_total, sweeps),
            out_shape=(pltpu.VMEM((2, 9, 4, 4, 4, 8, 128), F32), pltpu.VMEM((1, n_pts), F32)),
            in_specs=[any_spec, any_spec, vmem_spec, pl.BlockSpec(memory_space=pltpu.SMEM)],
            out_specs=(vmem_spec, vmem_spec),
            scratch_shapes=[
                pltpu.VMEM((n_pts, 512), BF16),
                pltpu.VMEM((4, 512, n_pts), F32),
                pltpu.VMEM((2, 512, PB), F32),
                pltpu.VMEM((2, 512, PB), F32),
                pltpu.VMEM((2, 9, 4, 4, 4, 8, 128), F32),
                pltpu.VMEM((2, 4, 4, 4, 4, 16, 128), BF16),
                pltpu.VMEM((2, 4, 4, 4, 8, 128), F32),
                pltpu.VMEM((2, 2, 512, 128), F32),
                pltpu.VMEM((2, 2, 512, 128), F32),
                pltpu.VMEM((4, 1, n_pts), F32),
                pltpu.VMEM((2, 4, 1, n_pts), F32),
                pltpu.VMEM((2, 1, n_pts), F32),
                pltpu.VMEM((1, n_pts), F32),
                *rbuf(0), *rbuf(1), *rbuf(2),
                pltpu.SemaphoreType.DMA((17,)),
                pltpu.SemaphoreType.DMA,
                pltpu.SemaphoreType.DMA((2,)),
                pltpu.SemaphoreType.DMA((2, 3, 15)),
                pltpu.SemaphoreType.DMA((2, 3, 15)),
                pltpu.SemaphoreType.DMA((2, 4, 15)),
                pltpu.SemaphoreType.DMA((2, 4, 15)),
            ],
            compiler_params=pltpu.CompilerParams(has_side_effects=True, collective_id=0, vmem_limit_bytes=61000000),
            cost_estimate=pl.CostEstimate(flops=6 * 2 * n_pts * 2048 * 512, bytes_accessed=1 << 24, transcendentals=0),
        )(points, mean_vecs.reshape(4, 4, 4, 2, 2, 8, 512), log_w.reshape(16, 128), inv_temp)
        out_mu, out_lw, out_lse = pl.pallas_call(
            write_out,
            out_shape=(jax.ShapeDtypeStruct((4, 4, 4, 2, 2, 8, 512), F32),
                       jax.ShapeDtypeStruct((16, 128), F32),
                       jax.ShapeDtypeStruct((1, n_pts), F32)),
            in_specs=[vmem_spec, vmem_spec],
            out_specs=(any_spec, vmem_spec, vmem_spec),
            scratch_shapes=[pltpu.SemaphoreType.DMA((16,))],
            compiler_params=pltpu.CompilerParams(vmem_limit_bytes=16 << 20),
        )(muf, lse)
        return out_mu.reshape(2048, 512), out_lw.reshape(2048), out_lse.reshape(n_pts)

    row_spec = P(("fit", "pts"))
    comp_spec = P(("fit", "comp"))
    return jax.shard_map(
        per_device,
        mesh=mesh,
        in_specs=(P(("fit", "pts"), None), P(("fit", "comp"), None), comp_spec, P()),
        out_specs=(P(("fit", "comp"), None), comp_spec, row_spec),
        check_vma=False,
    )
```

```python
import functools
import math

import jax
import jax.numpy as jnp
from jax import lax
from jax.experimental import pallas as pl
from jax.experimental.pallas import tpu as pltpu
from jax.sharding import PartitionSpec as P

PRIOR_ALPHA = 1e-3
COUNT_EPS = 1e-6
LOG2E = math.log2(math.e)
LN2 = math.log(2.0)
F32, BF16 = jnp.float32, jnp.bfloat16
MESH = pl.DeviceIdType.MESH

DIMS = ("z", "y", "x")
ORDERS = (("x", "y", "z"), ("y", "z", "x"), ("z", "x", "y"))
SUM_TILES = ((0, 3), (3, 6), (6, 9))
BF_TILES = (((0, 2), (2, 3), (3, 4)), ((0, 1), (1, 2), (2, 4)))
PB = 512
KC = 512


def cat(parts, axis):
    return jnp.concatenate(parts, axis=axis)


def kernel(n_total, k_total, sweeps, x_hbm, mean_hbm, lw_ref, beta_ref, muf, out_lse,
           xv, e_ref, l0, l1, s_ref, mu, ct, hrep, lrep, st, stp, wrow, qh,
           ra0, ra1, ra2, rb0, rb1, rb2, rc0, rc1, rc2,
           load_sem, ex_send, ex_recv, rs_send, rs_recv, ag_send, ag_recv):
    n_pts = xv.shape[0]
    nb = n_pts // PB
    fit, comp, pts = lax.axis_index("fit"), lax.axis_index("comp"), lax.axis_index("pts")
    me = {"z": lax.div(pts, 16), "y": lax.rem(lax.div(pts, 4), 4), "x": lax.rem(pts, 4)}
    near = {r: {d: lax.rem(me[d] + r, 4) for d in DIMS} for r in (1, 2, 3)}
    bufs = ((ra0, ra1, ra2), (rb0, rb1, rb2), (rc0, rc1, rc2))
    own = (me["z"], me["y"], me["x"])
    lane = lax.broadcasted_iota(jnp.int32, (8, 128), 1)

    def dev(d, r):
        c = {**me, d: near[r][d]}
        return (fit, comp, c["z"] * 16 + c["y"] * 4 + c["x"])

    def coord(d, r):
        return near[r][d] if r else me[d]

    def place(p, k, r, half=None):
        order = ORDERS[p]
        sel = {order[j]: me[order[j]] for j in range(k)}
        sel[order[k]] = coord(order[k], r)
        if half is not None:
            sel[order[2]] = pl.ds(2 * half, 2)
        return tuple(sel.get(d, slice(None)) for d in DIMS)

    def remote(src, dst, ss, rs, device):
        return pltpu.make_async_remote_copy(src_ref=src, dst_ref=dst, send_sem=ss, recv_sem=rs,
                                            device_id=device, device_id_type=MESH)

    def sums(h, p):
        return (h, pl.ds(SUM_TILES[p][0], SUM_TILES[p][1] - SUM_TILES[p][0]))

    def rs_copy(h, p, k, i):
        d, buf = ORDERS[p][k], bufs[k][p]
        if k >= 1:
            r = (1, 3, 2)[i]
            src = s_ref.at[sums(h, p) + place(p, k, r)]
        else:
            r = (1, 3, 1, 1, 3, 3)[i]
            if i in (2, 5):
                src = buf.at[h, 0 if i == 2 else 1]
            else:
                to, half = {0: (2, 0), 1: (2, 1), 3: (1, 1), 4: (3, 0)}[i]
                src = s_ref.at[sums(h, p) + place(p, k, to, half)]
        j = 6 * k + i
        return remote(src, buf.at[h, i], rs_send.at[h, p, j], rs_recv.at[h, p, j], dev(d, r))

    def rs_start(h, k, which=(0, 1, 3, 4)):
        for i in ((2, 0, 1) if k >= 1 else which):
            for p in range(3):
                rs_copy(h, p, k, i).start()

    def rs_relay(h, k):
        for p in range(3):
            buf = bufs[k][p]
            for i, to, half, nxt in ((0, 1, 0, 2), (1, 3, 1, 5)):
                rs_copy(h, p, k, i).wait_recv()
                buf[h, i] = buf[h, i] + s_ref[sums(h, p) + place(p, k, to, half)]
                rs_copy(h, p, k, nxt).start()

    def rs_finish(h, k):
        for p in range(3):
            buf = bufs[k][p]
            if k >= 1:
                for i in range(3):
                    rs_copy(h, p, k, i).wait()
                mine = sums(h, p) + place(p, k, 0)
                s_ref[mine] = (s_ref[mine] + buf[h, 0]) + (buf[h, 1] + buf[h, 2])
                continue
            for half, i, j in ((0, 2, 4), (1, 3, 5)):
                rs_copy(h, p, k, i).wait_recv()
                rs_copy(h, p, k, j).wait_recv()
                mine = sums(h, p) + place(p, k, 0, half)
                s_ref[mine] = s_ref[mine] + (buf[h, i] + buf[h, j])
            for i in range(6):
                rs_copy(h, p, k, i).wait_send()

    def bf_units(h):
        units = []
        for p, (lo, hi) in enumerate(BF_TILES[h]):
            units.append((mu, (h, pl.ds(lo, hi - lo)), p))
        return units + [(ct, (h,), 1)]

    def f32_units(h):
        return [(muf, sums(h, p), p) for p in range(3)]

    def ag_copy(units, h, u, k, i):
        ref, lead, p = units[u]
        d = ORDERS[p][k]
        if k >= 1:
            r = (1, 3, 2)[i]
            view = ref.at[lead + place(p, k, 0)]
        else:
            frm, half, r = ((0, 0, 1), (0, 1, 3), (0, 1, 1), (0, 0, 3), (3, 0, 1), (1, 1, 3))[i]
            view = ref.at[lead + place(p, k, frm, half)]
        j = 6 * k + i
        return remote(view, view, ag_send.at[h, u, j], ag_recv.at[h, u, j], dev(d, r))

    def ag_start(units, h, k):
        for i in ((2, 0, 1) if k >= 1 else range(4)):
            for u in range(len(units)):
                ag_copy(units, h, u, k, i).start()

    def ag_relay(units, h, k):
        for u in range(len(units)):
            for i, nxt in ((0, 4), (1, 5)):
                ag_copy(units, h, u, k, i).wait_recv()
                ag_copy(units, h, u, k, nxt).start()

    def ag_finish(units, h, k):
        for u in range(len(units)):
            if k >= 1:
                for i in range(3):
                    ag_copy(units, h, u, k, i).wait()
                continue
            for i in range(2, 6):
                ag_copy(units, h, u, k, i).wait_recv()
            for i in range(6):
                ag_copy(units, h, u, k, i).wait_send()

    def column(v, lanes):
        return jnp.broadcast_to(v[:, lanes:lanes + 1], (v.shape[0], 128))

    def expand(h):
        t = ct[h].reshape(512, 128)
        for hh in range(2):
            hrep[h, hh] = column(t, 32 * hh)
            lrep[h, hh] = column(t, 64 + 32 * hh) * LOG2E

    def logits(h, j, lref, b2):
        cols = pl.ds(pl.multiple_of(j * PB, PB), PB)
        xj = xv[cols, :]
        q = qh[:, cols]
        rows = cat([mu[h, c].reshape(1024, 128) for c in range(4)], 1)
        a = lax.dot_general(rows, xj, (((1,), (1,)), ((), ())), preferred_element_type=F32)
        a = a.reshape(64, 2, 8, PB)
        top = None
        for hh in range(2):
            hc = cat([hrep[h, hh]] * (PB // 128), 1)
            lc = cat([lrep[h, hh]] * (PB // 128), 1)
            v = ((a[:, hh].reshape(512, PB) - hc) - q) * b2 + lc
            lref[hh] = v
            t = jnp.max(v.reshape(64, 8, PB), axis=0)
            top = t if top is None else jnp.maximum(top, t)
        st[2 * h, :, cols] = jnp.max(top, axis=0, keepdims=True)

    def exps(h, j, lref):
        cols = pl.ds(pl.multiple_of(j * PB, PB), PB)
        m = st[2 * h, :, cols]
        tot = None
        for hh in range(2):
            e = jnp.exp2(lref[hh] - m)
            e_ref[2 * h + hh, :, cols] = e
            t = jnp.sum(e.reshape(64, 8, PB), axis=0)
            tot = t if tot is None else tot + t
        st[2 * h + 1, :, cols] = jnp.sum(tot, axis=0, keepdims=True)

    def scores(h, b2, during=()):
        logits(h, 0, l0, b2)

        @pl.loop(0, nb // 2 - 1)
        def _(i):
            for n, step in during:
                pl.when(i == n)(step)
            exps(h, 2 * i, l0)
            logits(h, 2 * i + 1, l1, b2)
            exps(h, 2 * i + 1, l1)
            logits(h, 2 * i + 2, l0, b2)

        logits(h, nb - 1, l1, b2)
        exps(h, nb - 2, l0)
        exps(h, nb - 1, l1)

    def normalise(slot):
        ex = remote(st, stp.at[slot], ex_send, ex_recv.at[slot], (fit, 1 - comp, pts))
        ex.start()
        for h in range(2):
            s_ref[h, 8] = jnp.zeros((4, 4, 4, 8, 128), F32)
        ex.wait()
        tops = [st[0], st[2], stp[slot, 0], stp[slot, 2]]
        mm = jnp.maximum(jnp.maximum(tops[0], tops[1]), jnp.maximum(tops[2], tops[3]))
        tot = (st[1] * jnp.exp2(tops[0] - mm) + st[3] * jnp.exp2(tops[1] - mm)) + (
            stp[slot, 1] * jnp.exp2(tops[2] - mm) + stp[slot, 3] * jnp.exp2(tops[3] - mm))
        lse2 = mm + jnp.log2(tot)
        for h in range(2):
            wrow[h] = jnp.exp2(tops[h] - lse2)
        return lse2

    def moments():
        @pl.loop(0, 4)
        def _(r4):
            h, hh = lax.div(r4, 2), lax.rem(r4, 2)
            pl.when(r4 == 2)(lambda: rs_start(0, 0))
            pl.when(r4 == 3)(lambda: rs_relay(0, 0))
            acc, cnt = None, None
            for kc in range(n_pts // KC):
                k0 = kc * KC
                r = e_ref[r4, :, k0:k0 + KC] * wrow[h, :, k0:k0 + KC]
                for t in range(KC // 128):
                    rt = r[:, t * 128:(t + 1) * 128]
                    cnt = rt if cnt is None else cnt + rt
                part = jnp.dot(r.astype(BF16), xv[k0:k0 + KC, :], preferred_element_type=F32)
                acc = part if acc is None else acc + part
            for c in range(4):
                s_ref[h, hh * 4 + c] = acc[:, c * 128:(c + 1) * 128].reshape(4, 4, 4, 8, 128)
            cb = jnp.broadcast_to(jnp.sum(cnt, axis=1, keepdims=True), (512, 128)).reshape(64, 8, 128)
            cb = jnp.where(lax.div(lane, 64) == hh, cb, 0.0)
            s_ref[h, 8] = s_ref[h, 8] + cb.reshape(4, 4, 4, 8, 128)

    def update(h):
        ntile = s_ref[(h, 8) + own]
        vals, tile = [], jnp.zeros((8, 128), F32)
        for hh in range(2):
            n = column(ntile, 64 * hh)
            row = [s_ref[(h, hh * 4 + c) + own] / (n + COUNT_EPS) for c in range(4)]
            vals.append(row)
            sq = (row[0] * row[0] + row[1] * row[1]) + (row[2] * row[2] + row[3] * row[3])
            hc = jnp.broadcast_to(0.5 * jnp.sum(sq, axis=1, keepdims=True), (8, 128))
            lw = jnp.log((n + PRIOR_ALPHA) / (n_total + k_total * PRIOR_ALPHA))
            tile = jnp.where(lax.div(lane, 32) == hh, hc, tile)
            tile = jnp.where(lax.div(lane, 32) == 2 + hh, lw, tile)
        return vals, tile

    def update_bf(h):
        vals, tile = update(h)
        for c in range(4):
            mu[(h, c) + own] = cat([vals[0][c], vals[1][c]], 0).astype(BF16)
        ct[(h,) + own] = tile

    def update_f32(h):
        vals, tile = update(h)
        for hh in range(2):
            for c in range(4):
                muf[(h, hh * 4 + c) + own] = vals[hh][c]
        muf[(h, 8) + own] = tile

    def exchange(units, upd):
        u0, u1 = units
        rs_start(1, 0, (0, 1))
        rs_finish(0, 0)
        rs_start(0, 1)
        rs_start(1, 0, (3, 4))
        rs_relay(1, 0)
        rs_finish(0, 1)
        rs_start(0, 2)
        rs_finish(0, 2)
        upd(0)
        ag_start(u0, 0, 2)
        rs_finish(1, 0)
        rs_start(1, 1)
        ag_finish(u0, 0, 2)
        ag_start(u0, 0, 1)
        rs_finish(1, 1)
        rs_start(1, 2)
        ag_finish(u0, 0, 1)
        ag_start(u0, 0, 0)
        rs_finish(1, 2)
        upd(1)
        ag_start(u1, 1, 2)
        ag_relay(u0, 0, 0)
        ag_finish(u1, 1, 2)
        ag_start(u1, 1, 1)
        ag_finish(u0, 0, 0)

    bar = pltpu.get_barrier_semaphore()
    pl.semaphore_signal(bar, inc=1, device_id=(fit, 1 - comp, pts), device_id_type=MESH)
    for d in DIMS:
        for r in (1, 2, 3):
            pl.semaphore_signal(bar, inc=1, device_id=dev(d, r), device_id_type=MESH)

    loads = [pltpu.make_async_copy(x_hbm, xv, load_sem.at[16])]
    for h in range(2):
        for hh in range(2):
            for c in range(4):
                t = hh * 4 + c
                loads.append(pltpu.make_async_copy(
                    mean_hbm.at[:, :, :, h, hh, :, pl.ds(c * 128, 128)], s_ref.at[h, t], load_sem.at[8 * h + t]))
    for c in loads[1:9] + loads[:1] + loads[9:]:
        c.start()
    st[...] = jnp.zeros_like(st)
    for i in range(16):
        col = jnp.broadcast_to(lw_ref[i:i + 1, :] * LOG2E, (128, 128)).T
        for g in range(4):
            for r4 in range(4):
                lo = 32 * g + 8 * r4
                lrep[r4 // 2, r4 % 2, (4 * i + g) * 8:(4 * i + g) * 8 + 8, :] = col[lo:lo + 8, :]
    loads[0].wait()

    @pl.loop(0, n_pts // 128, unroll=4)
    def _(i):
        rows = pl.ds(pl.multiple_of(i * 128, 128), 128)
        xb = xv[rows, :].astype(F32)
        sq = xb * xb
        sq = (sq[:, 0:128] + sq[:, 128:256]) + (sq[:, 256:384] + sq[:, 384:512])
        qh[:, rows] = jnp.sum(sq.T, axis=0, keepdims=True) * 0.5

    for c in loads[1:]:
        c.wait()

    @pl.loop(0, 2)
    def _(h):
        for hh in range(2):
            v = [s_ref[h, hh * 4 + c].reshape(512, 128) for c in range(4)]
            sq = (v[0] * v[0] + v[1] * v[1]) + (v[2] * v[2] + v[3] * v[3])
            hrep[h, hh] = jnp.broadcast_to(0.5 * jnp.sum(sq, axis=1, keepdims=True), (512, 128))
        for c in range(4):
            v = cat([s_ref[h, c].reshape(64, 8, 128), s_ref[h, 4 + c].reshape(64, 8, 128)], 1)
            mu[h, c] = v.astype(BF16).reshape(4, 4, 4, 16, 128)
        scores(h, beta_ref[0] * (2.0 * LOG2E))

    pl.semaphore_wait(bar, 10)

    bf = (bf_units(0), bf_units(1))

    @pl.loop(0, sweeps - 1)
    def _(sweep):
        b2 = beta_ref[sweep + 1] * (2.0 * LOG2E)
        normalise(lax.rem(sweep, 2))
        moments()
        exchange(bf, update_bf)
        expand(0)

        def next_phase():
            ag_finish(bf[1], 1, 1)
            ag_start(bf[1], 1, 0)

        scores(0, b2, ((0, next_phase), (2, lambda: ag_relay(bf[1], 1, 0))))
        ag_finish(bf[1], 1, 0)
        expand(1)
        scores(1, b2)

    out_lse[...] = normalise((sweeps - 1) % 2) * LN2
    moments()
    f32 = (f32_units(0), f32_units(1))
    exchange(f32, update_f32)
    ag_finish(f32[1], 1, 1)
    ag_start(f32[1], 1, 0)
    ag_relay(f32[1], 1, 0)
    ag_finish(f32[1], 1, 0)


def write_out(muf, lse, out_mu, out_lw, out_lse, sem):
    stores = []
    for h in range(2):
        for hh in range(2):
            for c in range(4):
                t = hh * 4 + c
                stores.append(pltpu.make_async_copy(
                    muf.at[h, t], out_mu.at[:, :, :, h, hh, :, pl.ds(c * 128, 128)], sem.at[8 * h + t]))
                stores[-1].start()
    for i in range(16):
        tiles = []
        for g in range(4):
            for r4 in range(4):
                v = muf[r4 // 2, 8, i // 4, i % 4, g]
                lo = 64 + 32 * (r4 % 2)
                tiles.append(jnp.broadcast_to(v[:, lo:lo + 1], (8, 128)))
        out_lw[i:i + 1, :] = cat(tiles, 0).T[0:1, :]
    out_lse[...] = lse[...]
    for c in stores:
        c.wait()


def solution(mesh):
    row_groups = mesh.shape["pts"]
    comp_groups = mesh.shape["comp"]

    def per_device(points, mean_vecs, log_w, inv_temp):
        n_pts = points.shape[0]
        n_total = n_pts * row_groups
        k_total = mean_vecs.shape[0] * comp_groups
        sweeps = inv_temp.shape[0]

        def rbuf(k):
            shapes = []
            for (lo, hi), order in zip(SUM_TILES, ORDERS):
                if k >= 1:
                    shapes.append(pltpu.VMEM((2, 3, hi - lo, *((4,) * (2 - k)), 8, 128), F32))
                    continue
                dims = [2 if d == order[2] else 4 for d in DIMS if d not in order[:k + 1]]
                shapes.append(pltpu.VMEM((2, 6, hi - lo, *dims, 8, 128), F32))
            return shapes

        any_spec = pl.BlockSpec(memory_space=pl.ANY)
        vmem_spec = pl.BlockSpec(memory_space=pltpu.VMEM)
        muf, lse = pl.pallas_call(
            functools.partial(kernel, n_total, k_total, sweeps),
            out_shape=(pltpu.VMEM((2, 9, 4, 4, 4, 8, 128), F32), pltpu.VMEM((1, n_pts), F32)),
            in_specs=[any_spec, any_spec, vmem_spec, pl.BlockSpec(memory_space=pltpu.SMEM)],
            out_specs=(vmem_spec, vmem_spec),
            scratch_shapes=[
                pltpu.VMEM((n_pts, 512), BF16),
                pltpu.VMEM((4, 512, n_pts), F32),
                pltpu.VMEM((2, 512, PB), F32),
                pltpu.VMEM((2, 512, PB), F32),
                pltpu.VMEM((2, 9, 4, 4, 4, 8, 128), F32),
                pltpu.VMEM((2, 4, 4, 4, 4, 16, 128), BF16),
                pltpu.VMEM((2, 4, 4, 4, 8, 128), F32),
                pltpu.VMEM((2, 2, 512, 128), F32),
                pltpu.VMEM((2, 2, 512, 128), F32),
                pltpu.VMEM((4, 1, n_pts), F32),
                pltpu.VMEM((2, 4, 1, n_pts), F32),
                pltpu.VMEM((2, 1, n_pts), F32),
                pltpu.VMEM((1, n_pts), F32),
                *rbuf(0), *rbuf(1), *rbuf(2),
                pltpu.SemaphoreType.DMA((17,)),
                pltpu.SemaphoreType.DMA,
                pltpu.SemaphoreType.DMA((2,)),
                pltpu.SemaphoreType.DMA((2, 3, 15)),
                pltpu.SemaphoreType.DMA((2, 3, 15)),
                pltpu.SemaphoreType.DMA((2, 4, 15)),
                pltpu.SemaphoreType.DMA((2, 4, 15)),
            ],
            compiler_params=pltpu.CompilerParams(has_side_effects=True, collective_id=0, vmem_limit_bytes=61000000),
            cost_estimate=pl.CostEstimate(flops=6 * 2 * n_pts * 2048 * 512, bytes_accessed=1 << 24, transcendentals=0),
        )(points, mean_vecs.reshape(4, 4, 4, 2, 2, 8, 512), log_w.reshape(16, 128), inv_temp)
        out_mu, out_lw, out_lse = pl.pallas_call(
            write_out,
            out_shape=(jax.ShapeDtypeStruct((4, 4, 4, 2, 2, 8, 512), F32),
                       jax.ShapeDtypeStruct((16, 128), F32),
                       jax.ShapeDtypeStruct((1, n_pts), F32)),
            in_specs=[vmem_spec, vmem_spec],
            out_specs=(any_spec, vmem_spec, vmem_spec),
            scratch_shapes=[pltpu.SemaphoreType.DMA((16,))],
            compiler_params=pltpu.CompilerParams(vmem_limit_bytes=16 << 20),
        )(muf, lse)
        return out_mu.reshape(2048, 512), out_lw.reshape(2048), out_lse.reshape(n_pts)

    row_spec = P(("fit", "pts"))
    comp_spec = P(("fit", "comp"))
    return jax.shard_map(
        per_device,
        mesh=mesh,
        in_specs=(P(("fit", "pts"), None), P(("fit", "comp"), None), comp_spec, P()),
        out_specs=(P(("fit", "comp"), None), comp_spec, row_spec),
        check_vma=False,
    )
```

```python
import functools
import math

import jax
import jax.numpy as jnp
from jax import lax
from jax.experimental import pallas as pl
from jax.experimental.pallas import tpu as pltpu
from jax.sharding import PartitionSpec as P

PRIOR_ALPHA = 1e-3
COUNT_EPS = 1e-6
LOG2E = math.log2(math.e)
LN2 = math.log(2.0)
F32, BF16 = jnp.float32, jnp.bfloat16
MESH = pl.DeviceIdType.MESH

DIMS = ("z", "y", "x")
ORDERS = (("x", "y", "z"), ("y", "z", "x"), ("z", "x", "y"))
SUM_TILES = ((0, 3), (3, 6), (6, 9))
BF_TILES = (((0, 2), (2, 3), (3, 4)), ((0, 1), (1, 2), (2, 4)))
PB = 512
KC = 512


def cat(parts, axis):
    return jnp.concatenate(parts, axis=axis)


def kernel(n_total, k_total, sweeps, x_hbm, mean_hbm, lw_ref, beta_ref, muf, out_lse,
           xv, e_ref, l0, l1, s_ref, mu, ct, hrep, lrep, st, stp, wrow, qh,
           ra0, ra1, ra2, rb0, rb1, rb2, rc0, rc1, rc2,
           load_sem, ex_send, ex_recv, rs_send, rs_recv, ag_send, ag_recv):
    n_pts = xv.shape[0]
    nb = n_pts // PB
    fit, comp, pts = lax.axis_index("fit"), lax.axis_index("comp"), lax.axis_index("pts")
    me = {"z": lax.div(pts, 16), "y": lax.rem(lax.div(pts, 4), 4), "x": lax.rem(pts, 4)}
    near = {r: {d: lax.rem(me[d] + r, 4) for d in DIMS} for r in (1, 2, 3)}
    bufs = ((ra0, ra1, ra2), (rb0, rb1, rb2), (rc0, rc1, rc2))
    own = (me["z"], me["y"], me["x"])
    lane = lax.broadcasted_iota(jnp.int32, (8, 128), 1)

    def dev(d, r):
        c = {**me, d: near[r][d]}
        return (fit, comp, c["z"] * 16 + c["y"] * 4 + c["x"])

    def coord(d, r):
        return near[r][d] if r else me[d]

    def place(p, k, r, half=None):
        order = ORDERS[p]
        sel = {order[j]: me[order[j]] for j in range(k)}
        sel[order[k]] = coord(order[k], r)
        if half is not None:
            sel[order[2]] = pl.ds(2 * half, 2)
        return tuple(sel.get(d, slice(None)) for d in DIMS)

    def remote(src, dst, ss, rs, device):
        return pltpu.make_async_remote_copy(src_ref=src, dst_ref=dst, send_sem=ss, recv_sem=rs,
                                            device_id=device, device_id_type=MESH)

    def sums(h, p):
        return (h, pl.ds(SUM_TILES[p][0], SUM_TILES[p][1] - SUM_TILES[p][0]))

    def rs_copy(h, p, k, i):
        d, buf = ORDERS[p][k], bufs[k][p]
        if k >= 1:
            r = (1, 3, 2)[i]
            src = s_ref.at[sums(h, p) + place(p, k, r)]
        else:
            r = (1, 3, 1, 1, 3, 3)[i]
            if i in (2, 5):
                src = buf.at[h, 0 if i == 2 else 1]
            else:
                to, half = {0: (2, 0), 1: (2, 1), 3: (1, 1), 4: (3, 0)}[i]
                src = s_ref.at[sums(h, p) + place(p, k, to, half)]
        j = 6 * k + i
        return remote(src, buf.at[h, i], rs_send.at[h, p, j], rs_recv.at[h, p, j], dev(d, r))

    def rs_start(h, k, which=(0, 1, 3, 4)):
        for i in ((2, 0, 1) if k >= 1 else which):
            for p in range(3):
                rs_copy(h, p, k, i).start()

    def rs_relay(h, k):
        for p in range(3):
            buf = bufs[k][p]
            for i, to, half, nxt in ((0, 1, 0, 2), (1, 3, 1, 5)):
                rs_copy(h, p, k, i).wait_recv()
                buf[h, i] = buf[h, i] + s_ref[sums(h, p) + place(p, k, to, half)]
                rs_copy(h, p, k, nxt).start()

    def rs_finish(h, k):
        for p in range(3):
            buf = bufs[k][p]
            if k >= 1:
                for i in range(3):
                    rs_copy(h, p, k, i).wait()
                mine = sums(h, p) + place(p, k, 0)
                s_ref[mine] = (s_ref[mine] + buf[h, 0]) + (buf[h, 1] + buf[h, 2])
                continue
            for half, i, j in ((0, 2, 4), (1, 3, 5)):
                rs_copy(h, p, k, i).wait_recv()
                rs_copy(h, p, k, j).wait_recv()
                mine = sums(h, p) + place(p, k, 0, half)
                s_ref[mine] = s_ref[mine] + (buf[h, i] + buf[h, j])
            for i in range(6):
                rs_copy(h, p, k, i).wait_send()

    def bf_units(h):
        units = []
        for p, (lo, hi) in enumerate(BF_TILES[h]):
            units.append((mu, (h, pl.ds(lo, hi - lo)), p))
        return units + [(ct, (h,), 1)]

    def f32_units(h):
        return [(muf, sums(h, p), p) for p in range(3)]

    def straight(units, k):
        return k >= 1 or units[0][0] is mu

    def ag_copy(units, h, u, k, i):
        ref, lead, p = units[u]
        d = ORDERS[p][k]
        if straight(units, k):
            r = (1, 3, 2)[i]
            view = ref.at[lead + place(p, k, 0)]
        else:
            frm, half, r = ((0, 0, 1), (0, 1, 3), (0, 1, 1), (0, 0, 3), (3, 0, 1), (1, 1, 3))[i]
            view = ref.at[lead + place(p, k, frm, half)]
        j = 6 * k + i
        return remote(view, view, ag_send.at[h, u, j], ag_recv.at[h, u, j], dev(d, r))

    def ag_start(units, h, k):
        for i in ((2, 0, 1) if straight(units, k) else range(4)):
            for u in range(len(units)):
                ag_copy(units, h, u, k, i).start()

    def ag_relay(units, h, k):
        if straight(units, k):
            return
        for u in range(len(units)):
            for i, nxt in ((0, 4), (1, 5)):
                ag_copy(units, h, u, k, i).wait_recv()
                ag_copy(units, h, u, k, nxt).start()

    def ag_finish(units, h, k):
        for u in range(len(units)):
            if straight(units, k):
                for i in range(3):
                    ag_copy(units, h, u, k, i).wait()
                continue
            for i in range(2, 6):
                ag_copy(units, h, u, k, i).wait_recv()
            for i in range(6):
                ag_copy(units, h, u, k, i).wait_send()

    def column(v, lanes):
        return jnp.broadcast_to(v[:, lanes:lanes + 1], (v.shape[0], 128))

    def expand(h):
        t = ct[h].reshape(512, 128)
        for hh in range(2):
            hrep[h, hh] = column(t, 32 * hh)
            lrep[h, hh] = column(t, 64 + 32 * hh) * LOG2E

    def logits(h, j, lref, b2):
        cols = pl.ds(pl.multiple_of(j * PB, PB), PB)
        xj = xv[cols, :]
        q = qh[:, cols]
        rows = cat([mu[h, c].reshape(1024, 128) for c in range(4)], 1)
        a = lax.dot_general(rows, xj, (((1,), (1,)), ((), ())), preferred_element_type=F32)
        a = a.reshape(64, 2, 8, PB)
        top = None
        for hh in range(2):
            hc = cat([hrep[h, hh]] * (PB // 128), 1)
            lc = cat([lrep[h, hh]] * (PB // 128), 1)
            v = ((a[:, hh].reshape(512, PB) - hc) - q) * b2 + lc
            lref[hh] = v
            t = jnp.max(v.reshape(64, 8, PB), axis=0)
            top = t if top is None else jnp.maximum(top, t)
        st[2 * h, :, cols] = jnp.max(top, axis=0, keepdims=True)

    def exps(h, j, lref):
        cols = pl.ds(pl.multiple_of(j * PB, PB), PB)
        m = st[2 * h, :, cols]
        tot = None
        for hh in range(2):
            e = jnp.exp2(lref[hh] - m)
            e_ref[2 * h + hh, :, cols] = e
            t = jnp.sum(e.reshape(64, 8, PB), axis=0)
            tot = t if tot is None else tot + t
        st[2 * h + 1, :, cols] = jnp.sum(tot, axis=0, keepdims=True)

    def scores(h, b2, during=()):
        logits(h, 0, l0, b2)

        @pl.loop(0, nb // 2 - 1)
        def _(i):
            for n, step in during:
                pl.when(i == n)(step)
            exps(h, 2 * i, l0)
            logits(h, 2 * i + 1, l1, b2)
            exps(h, 2 * i + 1, l1)
            logits(h, 2 * i + 2, l0, b2)

        logits(h, nb - 1, l1, b2)
        exps(h, nb - 2, l0)
        exps(h, nb - 1, l1)

    def normalise(slot):
        ex = remote(st, stp.at[slot], ex_send, ex_recv.at[slot], (fit, 1 - comp, pts))
        ex.start()
        for h in range(2):
            s_ref[h, 8] = jnp.zeros((4, 4, 4, 8, 128), F32)
        ex.wait()
        tops = [st[0], st[2], stp[slot, 0], stp[slot, 2]]
        mm = jnp.maximum(jnp.maximum(tops[0], tops[1]), jnp.maximum(tops[2], tops[3]))
        tot = (st[1] * jnp.exp2(tops[0] - mm) + st[3] * jnp.exp2(tops[1] - mm)) + (
            stp[slot, 1] * jnp.exp2(tops[2] - mm) + stp[slot, 3] * jnp.exp2(tops[3] - mm))
        lse2 = mm + jnp.log2(tot)
        for h in range(2):
            wrow[h] = jnp.exp2(tops[h] - lse2)
        return lse2

    def moments():
        @pl.loop(0, 4)
        def _(r4):
            h, hh = lax.div(r4, 2), lax.rem(r4, 2)
            pl.when(r4 == 2)(lambda: rs_start(0, 0))
            pl.when(r4 == 3)(lambda: rs_relay(0, 0))
            acc, cnt = None, None
            for kc in range(n_pts // KC):
                k0 = kc * KC
                r = e_ref[r4, :, k0:k0 + KC] * wrow[h, :, k0:k0 + KC]
                for t in range(KC // 128):
                    rt = r[:, t * 128:(t + 1) * 128]
                    cnt = rt if cnt is None else cnt + rt
                part = jnp.dot(r.astype(BF16), xv[k0:k0 + KC, :], preferred_element_type=F32)
                acc = part if acc is None else acc + part
            for c in range(4):
                s_ref[h, hh * 4 + c] = acc[:, c * 128:(c + 1) * 128].reshape(4, 4, 4, 8, 128)
            cb = jnp.broadcast_to(jnp.sum(cnt, axis=1, keepdims=True), (512, 128)).reshape(64, 8, 128)
            cb = jnp.where(lax.div(lane, 64) == hh, cb, 0.0)
            s_ref[h, 8] = s_ref[h, 8] + cb.reshape(4, 4, 4, 8, 128)

    def update(h):
        ntile = s_ref[(h, 8) + own]
        vals, tile = [], jnp.zeros((8, 128), F32)
        for hh in range(2):
            n = column(ntile, 64 * hh)
            row = [s_ref[(h, hh * 4 + c) + own] / (n + COUNT_EPS) for c in range(4)]
            vals.append(row)
            sq = (row[0] * row[0] + row[1] * row[1]) + (row[2] * row[2] + row[3] * row[3])
            hc = jnp.broadcast_to(0.5 * jnp.sum(sq, axis=1, keepdims=True), (8, 128))
            lw = jnp.log((n + PRIOR_ALPHA) / (n_total + k_total * PRIOR_ALPHA))
            tile = jnp.where(lax.div(lane, 32) == hh, hc, tile)
            tile = jnp.where(lax.div(lane, 32) == 2 + hh, lw, tile)
        return vals, tile

    def update_bf(h):
        vals, tile = update(h)
        for c in range(4):
            mu[(h, c) + own] = cat([vals[0][c], vals[1][c]], 0).astype(BF16)
        ct[(h,) + own] = tile

    def update_f32(h):
        vals, tile = update(h)
        for hh in range(2):
            for c in range(4):
                muf[(h, hh * 4 + c) + own] = vals[hh][c]
        muf[(h, 8) + own] = tile

    def exchange(units, upd):
        u0, u1 = units
        rs_start(1, 0, (0, 1))
        rs_finish(0, 0)
        rs_start(0, 1)
        rs_start(1, 0, (3, 4))
        rs_relay(1, 0)
        rs_finish(0, 1)
        rs_start(0, 2)
        rs_finish(0, 2)
        upd(0)
        ag_start(u0, 0, 2)
        rs_finish(1, 0)
        rs_start(1, 1)
        ag_finish(u0, 0, 2)
        ag_start(u0, 0, 1)
        rs_finish(1, 1)
        rs_start(1, 2)
        ag_finish(u0, 0, 1)
        ag_start(u0, 0, 0)
        rs_finish(1, 2)
        upd(1)
        ag_start(u1, 1, 2)
        ag_relay(u0, 0, 0)
        ag_finish(u1, 1, 2)
        ag_start(u1, 1, 1)
        ag_finish(u0, 0, 0)

    bar = pltpu.get_barrier_semaphore()
    pl.semaphore_signal(bar, inc=1, device_id=(fit, 1 - comp, pts), device_id_type=MESH)
    for d in DIMS:
        for r in (1, 2, 3):
            pl.semaphore_signal(bar, inc=1, device_id=dev(d, r), device_id_type=MESH)

    loads = [pltpu.make_async_copy(x_hbm, xv, load_sem.at[16])]
    for h in range(2):
        for hh in range(2):
            for c in range(4):
                t = hh * 4 + c
                loads.append(pltpu.make_async_copy(
                    mean_hbm.at[:, :, :, h, hh, :, pl.ds(c * 128, 128)], s_ref.at[h, t], load_sem.at[8 * h + t]))
    for c in loads[1:9] + loads[:1] + loads[9:]:
        c.start()
    st[...] = jnp.zeros_like(st)
    for i in range(16):
        col = jnp.broadcast_to(lw_ref[i:i + 1, :] * LOG2E, (128, 128)).T
        for g in range(4):
            for r4 in range(4):
                lo = 32 * g + 8 * r4
                lrep[r4 // 2, r4 % 2, (4 * i + g) * 8:(4 * i + g) * 8 + 8, :] = col[lo:lo + 8, :]
    loads[0].wait()

    @pl.loop(0, n_pts // 128, unroll=4)
    def _(i):
        rows = pl.ds(pl.multiple_of(i * 128, 128), 128)
        xb = xv[rows, :].astype(F32)
        sq = xb * xb
        sq = (sq[:, 0:128] + sq[:, 128:256]) + (sq[:, 256:384] + sq[:, 384:512])
        qh[:, rows] = jnp.sum(sq.T, axis=0, keepdims=True) * 0.5

    for c in loads[1:]:
        c.wait()

    @pl.loop(0, 2)
    def _(h):
        for hh in range(2):
            v = [s_ref[h, hh * 4 + c].reshape(512, 128) for c in range(4)]
            sq = (v[0] * v[0] + v[1] * v[1]) + (v[2] * v[2] + v[3] * v[3])
            hrep[h, hh] = jnp.broadcast_to(0.5 * jnp.sum(sq, axis=1, keepdims=True), (512, 128))
        for c in range(4):
            v = cat([s_ref[h, c].reshape(64, 8, 128), s_ref[h, 4 + c].reshape(64, 8, 128)], 1)
            mu[h, c] = v.astype(BF16).reshape(4, 4, 4, 16, 128)
        scores(h, beta_ref[0] * (2.0 * LOG2E))

    pl.semaphore_wait(bar, 10)

    bf = (bf_units(0), bf_units(1))

    @pl.loop(0, sweeps - 1)
    def _(sweep):
        b2 = beta_ref[sweep + 1] * (2.0 * LOG2E)
        normalise(lax.rem(sweep, 2))
        moments()
        exchange(bf, update_bf)
        expand(0)

        def next_phase():
            ag_finish(bf[1], 1, 1)
            ag_start(bf[1], 1, 0)

        scores(0, b2, ((0, next_phase),))
        ag_finish(bf[1], 1, 0)
        expand(1)
        scores(1, b2)

    out_lse[...] = normalise((sweeps - 1) % 2) * LN2
    moments()
    f32 = (f32_units(0), f32_units(1))
    exchange(f32, update_f32)
    ag_finish(f32[1], 1, 1)
    ag_start(f32[1], 1, 0)
    ag_relay(f32[1], 1, 0)
    ag_finish(f32[1], 1, 0)


def write_out(muf, lse, out_mu, out_lw, out_lse, sem):
    stores = []
    for h in range(2):
        for hh in range(2):
            for c in range(4):
                t = hh * 4 + c
                stores.append(pltpu.make_async_copy(
                    muf.at[h, t], out_mu.at[:, :, :, h, hh, :, pl.ds(c * 128, 128)], sem.at[8 * h + t]))
                stores[-1].start()
    for i in range(16):
        tiles = []
        for g in range(4):
            for r4 in range(4):
                v = muf[r4 // 2, 8, i // 4, i % 4, g]
                lo = 64 + 32 * (r4 % 2)
                tiles.append(jnp.broadcast_to(v[:, lo:lo + 1], (8, 128)))
        out_lw[i:i + 1, :] = cat(tiles, 0).T[0:1, :]
    out_lse[...] = lse[...]
    for c in stores:
        c.wait()


def solution(mesh):
    row_groups = mesh.shape["pts"]
    comp_groups = mesh.shape["comp"]

    def per_device(points, mean_vecs, log_w, inv_temp):
        n_pts = points.shape[0]
        n_total = n_pts * row_groups
        k_total = mean_vecs.shape[0] * comp_groups
        sweeps = inv_temp.shape[0]

        def rbuf(k):
            shapes = []
            for (lo, hi), order in zip(SUM_TILES, ORDERS):
                if k >= 1:
                    shapes.append(pltpu.VMEM((2, 3, hi - lo, *((4,) * (2 - k)), 8, 128), F32))
                    continue
                dims = [2 if d == order[2] else 4 for d in DIMS if d not in order[:k + 1]]
                shapes.append(pltpu.VMEM((2, 6, hi - lo, *dims, 8, 128), F32))
            return shapes

        any_spec = pl.BlockSpec(memory_space=pl.ANY)
        vmem_spec = pl.BlockSpec(memory_space=pltpu.VMEM)
        muf, lse = pl.pallas_call(
            functools.partial(kernel, n_total, k_total, sweeps),
            out_shape=(pltpu.VMEM((2, 9, 4, 4, 4, 8, 128), F32), pltpu.VMEM((1, n_pts), F32)),
            in_specs=[any_spec, any_spec, vmem_spec, pl.BlockSpec(memory_space=pltpu.SMEM)],
            out_specs=(vmem_spec, vmem_spec),
            scratch_shapes=[
                pltpu.VMEM((n_pts, 512), BF16),
                pltpu.VMEM((4, 512, n_pts), F32),
                pltpu.VMEM((2, 512, PB), F32),
                pltpu.VMEM((2, 512, PB), F32),
                pltpu.VMEM((2, 9, 4, 4, 4, 8, 128), F32),
                pltpu.VMEM((2, 4, 4, 4, 4, 16, 128), BF16),
                pltpu.VMEM((2, 4, 4, 4, 8, 128), F32),
                pltpu.VMEM((2, 2, 512, 128), F32),
                pltpu.VMEM((2, 2, 512, 128), F32),
                pltpu.VMEM((4, 1, n_pts), F32),
                pltpu.VMEM((2, 4, 1, n_pts), F32),
                pltpu.VMEM((2, 1, n_pts), F32),
                pltpu.VMEM((1, n_pts), F32),
                *rbuf(0), *rbuf(1), *rbuf(2),
                pltpu.SemaphoreType.DMA((17,)),
                pltpu.SemaphoreType.DMA,
                pltpu.SemaphoreType.DMA((2,)),
                pltpu.SemaphoreType.DMA((2, 3, 15)),
                pltpu.SemaphoreType.DMA((2, 3, 15)),
                pltpu.SemaphoreType.DMA((2, 4, 15)),
                pltpu.SemaphoreType.DMA((2, 4, 15)),
            ],
            compiler_params=pltpu.CompilerParams(has_side_effects=True, collective_id=0, vmem_limit_bytes=61000000),
            cost_estimate=pl.CostEstimate(flops=6 * 2 * n_pts * 2048 * 512, bytes_accessed=1 << 24, transcendentals=0),
        )(points, mean_vecs.reshape(4, 4, 4, 2, 2, 8, 512), log_w.reshape(16, 128), inv_temp)
        out_mu, out_lw, out_lse = pl.pallas_call(
            write_out,
            out_shape=(jax.ShapeDtypeStruct((4, 4, 4, 2, 2, 8, 512), F32),
                       jax.ShapeDtypeStruct((16, 128), F32),
                       jax.ShapeDtypeStruct((1, n_pts), F32)),
            in_specs=[vmem_spec, vmem_spec],
            out_specs=(any_spec, vmem_spec, vmem_spec),
            scratch_shapes=[pltpu.SemaphoreType.DMA((16,))],
            compiler_params=pltpu.CompilerParams(vmem_limit_bytes=16 << 20),
        )(muf, lse)
        return out_mu.reshape(2048, 512), out_lw.reshape(2048), out_lse.reshape(n_pts)

    row_spec = P(("fit", "pts"))
    comp_spec = P(("fit", "comp"))
    return jax.shard_map(
        per_device,
        mesh=mesh,
        in_specs=(P(("fit", "pts"), None), P(("fit", "comp"), None), comp_spec, P()),
        out_specs=(P(("fit", "comp"), None), comp_spec, row_spec),
        check_vma=False,
    )
```
